256 devices in a mesh: dp: 4 (over x), vocab: 64 (over y, z, core).
Axes of the slice: x: 4, y: 4, z: 8, core: 2. Of those that a mesh axis runs over, the one named last changes fastest.
Arguments:
- hidden: bfloat16 [1024, 8192], P('dp'), may hold values from -14 to 14
- weight: bfloat16 [8192, 65536], P('dp', 'vocab'), may hold values from -1 to 1, as said below
- targets: int32 [1024], P('dp'), may hold values from 0 to 65535
- cotangent: float32 [1024], P('dp'), may hold values from 1 to 8
Outputs:
- loss: float32 [1024], P('dp')
- grad_hidden: bfloat16 [1024, 8192], P('vocab', 'dp')
- grad_weight: bfloat16 [8192, 65536], P('dp', 'vocab')
The draws below stay inside these ranges and needn't reach their ends.
Inputs may be any that keep to these rules, and one draw needn't show every extreme that they name: `weight`: entries drawn with standard deviation 4 / sqrt(8192).
All inputs are finite; a program needn't handle non-finite values.
Results may differ from the reference program's by a relative error of at most 0.0047.
Values may be sent and summed in bfloat16 or wider, within the bound.
A program may use at most 128 MiB of HBM per device.

```python
import math
import jax
import jax.numpy as jnp
from jax import lax

D = 8192
VOCAB = 65536
TOKENS = 1024


def joint_draw(key):
    weight_key = jax.random.fold_in(key, 11)
    hidden_key = jax.random.fold_in(key, 12)
    weight = jnp.clip(jnp.clip(jax.random.normal(weight_key, (D, VOCAB), jnp.float32), -6.0, 6.0) * (4.0 / D ** 0.5), -1.0, 1.0)
    hidden = jnp.clip(jax.random.normal(hidden_key, (TOKENS, D), jnp.float32), -6.0, 6.0)
    return (weight, hidden)


def draw_weight(key, part):
    weight, hidden = joint_draw(key)
    return weight.astype(jnp.bfloat16)


def draw_hidden(key, part):
    weight, hidden = joint_draw(key)
    return hidden.astype(jnp.bfloat16)


def set_ends(result, key, smallest, top_value):
    longest = result.shape.index(max(result.shape))
    spots = []
    for shift in (0, 1):
        where = [jax.random.randint(jax.random.fold_in(key, axis), (), 0, length) for axis, length in enumerate(result.shape)]
        where[longest] = (where[longest] + shift) % result.shape[longest]
        spots.append(tuple(where))
    return result.at[spots[0]].set(smallest).at[spots[1]].set(top_value)


def shard_levels(own_key, dims, split, smallest, top_value):
    def one(position, shards_of):
        steps = jax.random.uniform(jax.random.fold_in(jax.random.fold_in(own_key, 6), position), (shards_of,), jnp.float32, smallest / len(split), top_value / len(split))
        return jnp.repeat(jnp.exp(steps), dims[position] // shards_of).reshape((-1,) + (1,) * (len(dims) - position - 1))

    gain = one(*split[0])
    for cut in split[1:]:
        gain = gain * one(*cut)
    return gain


def setup_inputs(seed: int = 0) -> dict:
    key_list = jax.random.split(jax.random.key(seed), 5)
    return {
        "hidden": draw_hidden(jax.random.fold_in(key_list[4], 71), 0),
        "weight": draw_weight(jax.random.fold_in(key_list[4], 71), 0),
        "targets": set_ends(jax.random.randint(key_list[2], (TOKENS,), 0, VOCAB), jax.random.fold_in(key_list[2], 1), 0, VOCAB - 1).astype(jnp.int32),
        "cotangent": jnp.clip(jnp.exp(math.log(8.0) - 2.0794415 * jax.random.uniform(key_list[3], (TOKENS,), jnp.float32) ** shard_levels(key_list[3], (TOKENS,), ((0, 4),), -0.2, 0.2)), 1.0, 8.0),
    }


def reference(hidden, weight, targets, cotangent):
    logits = jnp.dot(hidden, weight, preferred_element_type=jnp.float32)
    row_max = jnp.max(logits, axis=1, keepdims=True)
    shifted = jnp.exp(logits - row_max)
    sum_exp = jnp.sum(shifted, axis=1, keepdims=True)
    columns = jnp.arange(VOCAB, dtype=jnp.int32)
    onehot = (targets.astype(jnp.int32)[:, None] == columns[None, :]).astype(jnp.float32)
    picked = jnp.sum(logits * onehot, axis=1)
    loss = row_max[:, 0] + jnp.log(sum_exp[:, 0]) - picked
    grad_logits = (cotangent[:, None] * (shifted / sum_exp - onehot)).astype(jnp.bfloat16)
    grad_hidden = lax.dot_general(grad_logits, weight, (((1,), (1,)), ((), ())), preferred_element_type=jnp.float32).astype(jnp.bfloat16)
    grad_weight = lax.dot_general(hidden, grad_logits, (((0,), (0,)), ((), ())), preferred_element_type=jnp.float32).astype(jnp.bfloat16)
    return (loss, grad_hidden, grad_weight)
```

```python
import jax
import jax.numpy as jnp
from jax import lax
from jax.experimental import pallas as pl
from jax.experimental.pallas import tpu as pltpu
from jax.sharding import PartitionSpec as P

F32, BF16, I16 = jnp.float32, jnp.bfloat16, jnp.int16
NX, NY, NZ = 4, 4, 8
FINE = 64.0 / 0.6931471805599453
TOP = 32700.0
NEG = (((1,), (1,)), ((), ()))


def row_code(x):
    top = jnp.max(jnp.abs(x), axis=1, keepdims=True)
    return jnp.ceil(jnp.log(jnp.maximum(top, 1e-30)) * FINE)


def pack_tall(x, dst):
    rows, cols = x.shape
    k = row_code(x)
    inv = jnp.exp(k * (-1.0 / FINE)) * TOP
    for j in range(cols // 128):
        dst[j * rows : (j + 1) * rows, :] = jnp.round(x[:, j * 128 : (j + 1) * 128] * inv).astype(I16)
    line = jnp.broadcast_to(k, (rows, 128)).T[0:1, :]
    dst[cols // 128 * rows : cols // 128 * rows + 16, :] = jnp.broadcast_to(line, (16, 128)).astype(I16)


def unpack_tall(src, rows, cols):
    at = cols // 128 * rows
    line = src[at : at + 16, :].astype(F32)[0:1, :]
    k = jnp.broadcast_to(line, (rows, rows)).T
    scale = jnp.exp(k * (1.0 / FINE)) * (1.0 / TOP)
    return jnp.concatenate(
        [src[j * rows : (j + 1) * rows, :].astype(F32) * scale for j in range(cols // 128)], axis=1
    )


def pack_flat(x, dst):
    rows, cols = x.shape
    k = row_code(x)
    inv = jnp.exp(k * (-1.0 / FINE)) * TOP
    for j in range(cols // 128):
        dst[j * rows : (j + 1) * rows, :] = jnp.round(x[:, j * 128 : (j + 1) * 128] * inv).astype(I16)
    dst[cols // 128 * rows : (cols // 128 + 1) * rows, :] = jnp.broadcast_to(k, (rows, 128)).astype(I16)


def unpack_flat(src, rows, cols):
    at = cols // 128 * rows
    scale = jnp.exp(src[at : at + rows, :].astype(F32) * (1.0 / FINE)) * (1.0 / TOP)
    return jnp.concatenate(
        [src[j * rows : (j + 1) * rows, :].astype(F32) * scale for j in range(cols // 128)], axis=1
    )


def as_column(line):
    n = line.shape[1]
    return jnp.broadcast_to(line, (128, n)).T[:, 0:1]


def as_line(column):
    n = column.shape[0]
    return jnp.broadcast_to(column, (n, 128)).T[0:1, :]


def kernel(
    hid, w, tgt, cot, loss, gh, gw,
    hbuf, wbuf, pb, sx, rx, st, gall, gt, rb, zs, zr, fin, ys, yr, wst,
    lsem, hs, hr, xs, xr, ss, sr, gs, gr, ds_, dr, zss, zrs, yss, yrs, ws,
):
    x = lax.axis_index("dp")
    v = lax.axis_index("vocab")
    y, z, c = v // (2 * NZ), (v // 2) % NZ, v % 2
    oc = 1 - c

    def dev(dx=0, dy=0, dz=0, core=None):
        yy, zz = (y + dy) % NY, (z + dz) % NZ
        cc = c if core is None else core
        return {"dp": (x + dx) % NX, "vocab": (yy * NZ + zz) * 2 + cc}

    def remote(src, dst, send, recv, to):
        return pltpu.make_async_remote_copy(
            src_ref=src, dst_ref=dst, send_sem=send, recv_sem=recv,
            device_id=to, device_id_type=pl.DeviceIdType.MESH,
        )

    local = [pltpu.make_async_copy(w.at[pl.ds(h * 1024, 1024), :], wbuf.at[h], lsem.at[h]) for h in range(2)]
    for h in range(2):
        cols = pl.multiple_of(x * 2048 + h * 1024, 1024)
        local.append(pltpu.make_async_copy(hid.at[:, pl.ds(cols, 1024)], hbuf.at[h, 0], lsem.at[2 + h]))
    for d in local:
        d.start()

    barrier = pltpu.get_barrier_semaphore()
    peers = [dev(dx=k) for k in (1, 2, 3)] + [dev(core=oc)]
    peers += [dev(dy=k) for k in (1, 2, 3)] + [dev(dz=k) for k in range(1, NZ)]
    for p in peers:
        pl.semaphore_signal(barrier, inc=1, device_id=p, device_id_type=pl.DeviceIdType.MESH)
    pl.semaphore_wait(barrier, len(peers))

    order = (2, 1, 3)
    sent = []
    mine = pl.ds(pl.multiple_of(y * 64, 64), 64)
    take = {}
    for r in order:
        to = (4 - r) % 4
        cols = pl.multiple_of(((x + to) % NX) * 2048 + c * 1024, 1024)
        take[r] = remote(hid.at[mine, pl.ds(cols, 1024)], hbuf.at[c, r, mine, :], hs.at[r, 0], hr.at[r, 0], dev(dx=to))
        take[r].start()
        sent.append(take[r])
    around = {}
    for r in order:
        take[r].wait_recv()
        for k, dy in ((1, 1), (2, -1)):
            d = remote(hbuf.at[c, r, mine, :], hbuf.at[c, r, mine, :], hs.at[r, k], hr.at[r, k], dev(dy=dy))
            d.start()
            around[r, k] = d
            sent.append(d)

    for d in local:
        d.wait()

    def product(r):
        def step(n, carry):
            at = pl.ds(pl.multiple_of(n * 256, 256), 256)
            pb[r, :, at] = jnp.dot(hbuf[0, r], wbuf[0, :, at], preferred_element_type=F32) + jnp.dot(
                hbuf[1, r], wbuf[1, :, at], preferred_element_type=F32
            )
            return carry

        lax.fori_loop(0, 4, step, 0)

    product(0)

    def forward(r):
        around[r, 1].wait_recv()
        rows = pl.ds(pl.multiple_of(((y + 3) % NY) * 64, 64), 32)
        d = remote(hbuf.at[c, r, rows, :], hbuf.at[c, r, rows, :], hs.at[r, 3], hr.at[r, 3], dev(dy=1))
        d.start()
        around[r, 3] = d
        around[r, 2].wait_recv()
        rows = pl.ds(pl.multiple_of(((y + 1) % NY) * 64 + 32, 32), 32)
        e = remote(hbuf.at[c, r, rows, :], hbuf.at[c, r, rows, :], hs.at[r, 4], hr.at[r, 4], dev(dy=-1))
        e.start()
        around[r, 4] = e
        sent.extend((d, e))

    across = {}

    def share(r):
        around[r, 3].wait_recv()
        around[r, 4].wait_recv()
        d = remote(hbuf.at[c, r], hbuf.at[c, r], hs.at[r, 5], hr.at[r, 5], dev(core=oc))
        d.start()
        across[r] = d
        sent.append(d)

    RIGHT, LEFT = 1, -1
    ring = {}

    def send_x(k, dx):
        d = remote(sx.at[k], rx.at[k], xs.at[k], xr.at[k], dev(dx=dx))
        d.start()
        ring[k] = d
        sent.append(d)

    top, low = slice(0, 128), slice(128, 256)
    forward(2)
    forward(1)
    share(2)
    forward(3)
    share(1)
    across[2].wait_recv()
    product(2)
    pack_tall(pb[2, top, :], sx.at[0])
    send_x(0, RIGHT)
    pack_tall(pb[2, low, :], sx.at[1])
    send_x(1, LEFT)
    share(3)
    across[1].wait_recv()
    product(1)
    pack_tall(pb[1, low, :], sx.at[2])
    send_x(2, RIGHT)
    across[3].wait_recv()
    product(3)
    pack_tall(pb[3, top, :], sx.at[3])
    send_x(3, LEFT)
    ring[0].wait_recv()
    pack_tall(pb[1, top, :] + unpack_tall(rx.at[0], 128, 1024), sx.at[4])
    send_x(4, RIGHT)
    ring[1].wait_recv()
    pack_tall(pb[3, low, :] + unpack_tall(rx.at[1], 128, 1024), sx.at[5])
    send_x(5, LEFT)
    ring[2].wait_recv()
    pb[0, low, :] += unpack_tall(rx.at[2], 128, 1024)
    ring[3].wait_recv()
    pb[0, top, :] += unpack_tall(rx.at[3], 128, 1024)
    ring[4].wait_recv()
    pb[0, top, :] += unpack_tall(rx.at[4], 128, 1024)
    ring[5].wait_recv()
    pb[0, low, :] += unpack_tall(rx.at[5], 128, 1024)

    target = as_column(tgt[...].astype(F32))
    weigh = as_column(cot[...])
    first = (v * 1024).astype(F32)
    lanes = lax.broadcasted_iota(jnp.int32, (128, 1024), 1).astype(F32) + first
    tops, sums, picks = [], [], []
    for half in (top, low):
        logit = pb[0, half, :]
        m = jnp.max(logit, axis=1, keepdims=True)
        hot = lanes == target[half]
        picks.append(jnp.sum(jnp.where(hot, logit, 0.0), axis=1, keepdims=True))
        e = jnp.exp(logit - m)
        pb[0, half, :] = e
        tops.append(m)
        sums.append(jnp.sum(e, axis=1, keepdims=True))
    own_top = jnp.concatenate(tops, axis=0)
    st[0, 0, 0:1, :] = as_line(own_top)
    st[0, 0, 1:2, :] = as_line(jnp.concatenate(sums, axis=0))
    st[0, 0, 2:3, :] = as_line(jnp.concatenate(picks, axis=0))

    def join(level, places, out):
        for k, p in enumerate(places, 1):
            d = remote(st.at[level, 0], st.at[level, k], ss.at[level, k], sr.at[level, k], p)
            d.start()
            sent.append(d)
            places[k - 1] = d
        for d in places:
            d.wait_recv()
        n = len(places) + 1
        m = st[level, 0, 0:1, :]
        for k in range(1, n):
            m = jnp.maximum(m, st[level, k, 0:1, :])
        s = jnp.zeros_like(m)
        q = jnp.zeros_like(m)
        for k in range(n):
            s = s + st[level, k, 1:2, :] * jnp.exp(st[level, k, 0:1, :] - m)
            q = q + st[level, k, 2:3, :]
        st[out, 0, 0:1, :] = m
        st[out, 0, 1:2, :] = s
        st[out, 0, 2:3, :] = q
        return m, s, q

    join(0, [dev(core=oc)], 1)
    join(1, [dev(dz=k) for k in range(1, NZ)], 2)
    m, s, q = join(2, [dev(dy=k) for k in (1, 2, 3)], 3)
    loss[...] = m + jnp.log(s) - q
    all_top, all_sum = as_column(m), as_column(s)
    for i, half in enumerate((top, low)):
        factor = jnp.exp(own_top[half] - all_top[half]) / all_sum[half]
        hot = (lanes == target[half]).astype(F32)
        gall[0, half, :] = (weigh[half] * (pb[0, half, :] * factor - hot)).astype(BF16)

    def send_g(k, src, dst, half, dx):
        d = remote(gall.at[src, half, :], gall.at[dst, half, :], gs.at[k], gr.at[k], dev(dx=dx))
        d.start()
        sent.append(d)
        return d

    T, L = pl.ds(0, 128), pl.ds(128, 128)
    a0 = send_g(0, 0, 3, T, RIGHT)
    b0 = send_g(1, 0, 1, L, LEFT)
    a1 = send_g(2, 0, 3, L, RIGHT)
    b1 = send_g(3, 0, 1, T, LEFT)

    pair, zd = {}, {}

    def block_product(r):
        for h in range(2):
            def step(n, carry, h=h):
                at = pl.ds(pl.multiple_of(n * 256, 256), 256)
                out = pl.ds(pl.multiple_of(n * 256 + h * 1024, 256), 256)
                res = lax.dot_general(gall[r], wbuf[h, at, :], NEG, preferred_element_type=F32)
                gt[r, :, :, :, out] = res.reshape(NZ, 2, 16, 256)
                return carry

            lax.fori_loop(0, 4, step, 0)
        d = remote(gt.at[r, :, oc], rb.at[r], ds_.at[r], dr.at[r], dev(core=oc))
        d.start()
        pair[r] = d
        sent.append(d)

    def piece(r, k):
        zz = (z + k) % NZ
        return gt[r, zz, c] + rb[r, zz]

    def send_z(r, d, k, rows):
        cp = remote(
            zs.at[r, d, k, pl.ds(0, rows), :], zr.at[r, d, k, pl.ds(0, rows), :],
            zss.at[r, d, k], zrs.at[r, d, k], dev(dz=1 if d == 0 else -1),
        )
        cp.start()
        zd[r, d, k] = cp
        sent.append(cp)

    def z_step(r, k):
        if k == 0:
            pair[r].wait_recv()
            far = piece(r, 4)
            pack_flat(far[:, :1024], zs.at[r, 0, 0])
            send_z(r, 0, 0, 144)
            pack_flat(far[:, 1024:], zs.at[r, 1, 0])
            send_z(r, 1, 0, 144)
        elif k < 4:
            for d in range(2):
                val = piece(r, 4 - k if d == 0 else 4 + k)
                zd[r, d, k - 1].wait_recv()
                got = zr.at[r, d, k - 1]
                if k == 1:
                    part = unpack_flat(got, 16, 1024)
                    none = jnp.zeros_like(part)
                    val = val + jnp.concatenate([part, none] if d == 0 else [none, part], axis=1)
                else:
                    val = val + unpack_flat(got, 16, 2048)
                pack_flat(val, zs.at[r, d, k])
                send_z(r, d, k, 272)
        else:
            val = piece(r, 0)
            for d in range(2):
                zd[r, d, 3].wait_recv()
                val = val + unpack_flat(zr.at[r, d, 3], 16, 2048)
            fin[r] = val

    def weight_tile(f):
        h, at = f // 4, pl.ds((f % 4) * 256, 256)
        lhs = hbuf[h, :, :, at].reshape(1024, 256)
        rhs = gall[...].reshape(1024, 1024)
        out = lax.dot_general(lhs, rhs, (((0,), (0,)), ((), ())), preferred_element_type=F32)
        wst[f] = out.astype(BF16)
        d = pltpu.make_async_copy(wst.at[f], gw.at[pl.ds(f * 256, 256), :], ws.at[f])
        d.start()
        return d

    block_product(0)
    a0.wait_recv()
    f0 = send_g(4, 3, 2, T, RIGHT)
    b0.wait_recv()
    f1 = send_g(5, 1, 2, L, LEFT)
    z_step(0, 0)
    z_step(0, 1)
    a1.wait_recv()
    block_product(3)
    z_step(0, 2)
    b1.wait_recv()
    block_product(1)
    z_step(3, 0)
    z_step(0, 3)
    z_step(1, 0)
    z_step(3, 1)
    z_step(0, 4)
    f0.wait_recv()
    f1.wait_recv()
    block_product(2)
    z_step(1, 1)
    z_step(3, 2)
    z_step(2, 0)
    tiles = [weight_tile(0)]
    z_step(1, 2)
    z_step(3, 3)
    tiles.append(weight_tile(1))
    z_step(2, 1)
    z_step(3, 4)
    z_step(1, 3)
    tiles.append(weight_tile(2))
    z_step(2, 2)
    z_step(1, 4)
    tiles.append(weight_tile(3))
    tiles.append(weight_tile(4))
    z_step(2, 3)
    tiles.append(weight_tile(5))
    z_step(2, 4)

    def held(k):
        return fin[(y + k - x + NX) % NX]

    def send_y(k, rows, dy):
        d = remote(ys.at[k, pl.ds(0, rows), :], yr.at[k, pl.ds(0, rows), :], yss.at[k], yrs.at[k], dev(dy=dy))
        d.start()
        sent.append(d)
        return d

    far = held(2)
    pack_flat(far[:, :1024], ys.at[0])
    y0 = send_y(0, 144, 1)
    pack_flat(far[:, 1024:], ys.at[1])
    y1 = send_y(1, 144, -1)
    tiles.append(weight_tile(6))
    none = jnp.zeros((16, 1024), F32)
    y0.wait_recv()
    pack_flat(held(1) + jnp.concatenate([unpack_flat(yr.at[0], 16, 1024), none], axis=1), ys.at[2])
    y2 = send_y(2, 272, 1)
    y1.wait_recv()
    pack_flat(held(3) + jnp.concatenate([none, unpack_flat(yr.at[1], 16, 1024)], axis=1), ys.at[3])
    y3 = send_y(3, 272, -1)
    tiles.append(weight_tile(7))
    y2.wait_recv()
    y3.wait_recv()
    gh[...] = (held(0) + unpack_flat(yr.at[2], 16, 2048) + unpack_flat(yr.at[3], 16, 2048)).astype(BF16)

    for d in sent:
        d.wait_send()
    for d in tiles:
        d.wait()


def shards(hidden, weight, targets, cotangent):
    vm, dma = pltpu.VMEM, pltpu.SemaphoreType.DMA
    space = pl.BlockSpec(memory_space=pltpu.VMEM)
    raw = pl.BlockSpec(memory_space=pl.ANY)
    loss, gh, gw = pl.pallas_call(
        kernel,
        out_shape=(
            jax.ShapeDtypeStruct((1, 256), F32),
            jax.ShapeDtypeStruct((16, 2048), BF16),
            jax.ShapeDtypeStruct((2048, 1024), BF16),
        ),
        in_specs=[raw, raw, space, space],
        out_specs=(space, space, raw),
        scratch_shapes=[
            vm((2, 4, 256, 1024), BF16),
            vm((2, 1024, 1024), BF16),
            vm((4, 256, 1024), F32),
            vm((6, 1040, 128), I16),
            vm((6, 1040, 128), I16),
            vm((4, 8, 8, 256), F32),
            vm((4, 256, 1024), BF16),
            vm((4, NZ, 2, 16, 2048), F32),
            vm((4, NZ, 16, 2048), F32),
            vm((4, 2, 4, 272, 128), I16),
            vm((4, 2, 4, 272, 128), I16),
            vm((4, 16, 2048), F32),
            vm((4, 272, 128), I16),
            vm((4, 272, 128), I16),
            vm((8, 256, 1024), BF16),
            dma((4,)), dma((4, 6)), dma((4, 6)), dma((6,)), dma((6,)),
            dma((3, 8)), dma((3, 8)), dma((6,)), dma((6,)), dma((4,)), dma((4,)),
            dma((4, 2, 4)), dma((4, 2, 4)), dma((4,)), dma((4,)), dma((8,)),
        ],
        compiler_params=pltpu.CompilerParams(
            collective_id=0, has_side_effects=True, vmem_limit_bytes=60 * 1024 * 1024
        ),
    )(hidden, weight, targets.reshape(1, 256), cotangent.reshape(1, 256))
    return loss.reshape(256), gh, gw


def solution(mesh):
    in_specs = (P("dp", None), P("dp", "vocab"), P("dp"), P("dp"))
    out_specs = (P("dp"), P("vocab", "dp"), P("dp", "vocab"))
    return jax.shard_map(shards, mesh=mesh, in_specs=in_specs, out_specs=out_specs, check_vma=False)
```

```python
import jax
import jax.numpy as jnp
from jax import lax
from jax.experimental import pallas as pl
from jax.experimental.pallas import tpu as pltpu
from jax.sharding import PartitionSpec as P

F32, BF16, I16 = jnp.float32, jnp.bfloat16, jnp.int16
NX, NY, NZ = 4, 4, 8
FINE = 64.0 / 0.6931471805599453
TOP = 32700.0


def row_code(x):
    top = jnp.max(jnp.abs(x), axis=1, keepdims=True)
    return jnp.ceil(jnp.log(jnp.maximum(top, 1e-30)) * FINE)


def pack_tall(x, dst):
    rows, cols = x.shape
    k = row_code(x)
    inv = jnp.exp(k * (-1.0 / FINE)) * TOP
    for j in range(cols // 128):
        dst[j * rows : (j + 1) * rows, :] = jnp.round(x[:, j * 128 : (j + 1) * 128] * inv).astype(I16)
    line = jnp.broadcast_to(k, (rows, 128)).T[0:1, :]
    dst[cols // 128 * rows : cols // 128 * rows + 16, :] = jnp.broadcast_to(line, (16, 128)).astype(I16)


def unpack_tall(src, rows, cols):
    at = cols // 128 * rows
    line = src[at : at + 16, :].astype(F32)[0:1, :]
    k = jnp.broadcast_to(line, (rows, rows)).T
    scale = jnp.exp(k * (1.0 / FINE)) * (1.0 / TOP)
    return jnp.concatenate(
        [src[j * rows : (j + 1) * rows, :].astype(F32) * scale for j in range(cols // 128)], axis=1
    )


def pack_flat(x, dst):
    rows, cols = x.shape
    k = row_code(x)
    inv = jnp.exp(k * (-1.0 / FINE)) * TOP
    for j in range(cols // 128):
        dst[j * rows : (j + 1) * rows, :] = jnp.round(x[:, j * 128 : (j + 1) * 128] * inv).astype(I16)
    dst[cols // 128 * rows : (cols // 128 + 1) * rows, :] = jnp.broadcast_to(k, (rows, 128)).astype(I16)


def unpack_flat(src, rows, cols):
    at = cols // 128 * rows
    scale = jnp.exp(src[at : at + rows, :].astype(F32) * (1.0 / FINE)) * (1.0 / TOP)
    return jnp.concatenate(
        [src[j * rows : (j + 1) * rows, :].astype(F32) * scale for j in range(cols // 128)], axis=1
    )


def as_column(line):
    n = line.shape[1]
    return jnp.broadcast_to(line, (128, n)).T[:, 0:1]


def as_line(column):
    n = column.shape[0]
    return jnp.broadcast_to(column, (n, 128)).T[0:1, :]


def kernel(
    hid, w, tgt_in, cot_in, loss, gh, gw,
    tgt, cot,    hbuf, wbuf, wt, pb, sx, rx, st, eb, fx, gall, gt, rb, zs, zr, fin, ys, yr,
    lsem, hs, hr, xs, xr, ss, sr, gs, gr, fs, fr, ds_, dr, zss, zrs, yss, yrs,
):
    x = lax.axis_index("dp")
    v = lax.axis_index("vocab")
    y, z, c = v // (2 * NZ), (v // 2) % NZ, v % 2
    oc = 1 - c

    def dev(dx=0, dy=0, dz=0, core=None):
        yy, zz = (y + dy) % NY, (z + dz) % NZ
        cc = c if core is None else core
        return {"dp": (x + dx) % NX, "vocab": (yy * NZ + zz) * 2 + cc}

    def remote(src, dst, send, recv, to):
        return pltpu.make_async_remote_copy(
            src_ref=src, dst_ref=dst, send_sem=send, recv_sem=recv,
            device_id=to, device_id_type=pl.DeviceIdType.MESH,
        )

    local = [pltpu.make_async_copy(w.at[pl.ds(h * 1024, 1024), :], wbuf.at[h], lsem.at[h]) for h in range(2)]
    for h in range(2):
        cols = pl.multiple_of(x * 2048 + h * 1024, 1024)
        local.append(pltpu.make_async_copy(hid.at[:, pl.ds(cols, 1024)], hbuf.at[h, 0], lsem.at[2 + h]))
    local.append(pltpu.make_async_copy(tgt_in, tgt, lsem.at[4]))
    local.append(pltpu.make_async_copy(cot_in, cot, lsem.at[5]))
    for d in local:
        d.start()

    barrier = pltpu.get_barrier_semaphore()
    peers = [dev(dx=k) for k in (1, 2, 3)] + [dev(core=oc)]
    peers += [dev(dy=k) for k in (1, 2, 3)] + [dev(dz=k) for k in range(1, NZ)]
    for p in peers:
        pl.semaphore_signal(barrier, inc=1, device_id=p, device_id_type=pl.DeviceIdType.MESH)
    pl.semaphore_wait(barrier, len(peers))

    sent = []
    mine = pl.ds(pl.multiple_of(y * 64, 64), 64)
    take = {}
    def columns_for(r):
        to = (4 - r) % 4
        return to, pl.ds(pl.multiple_of(((x + to) % NX) * 2048 + c * 1024, 1024), 1024)

    to, cols = columns_for(2)
    take[2] = remote(hid.at[mine, cols], hbuf.at[c, 2, mine, :], hs.at[2, 0], hr.at[2, 0], dev(dx=to))
    take[2].start()
    sent.append(take[2])

    def direct(r):
        to, cols = columns_for(r)
        take[r] = remote(hid.at[:, cols], hbuf.at[c, r], hs.at[r, 0], hr.at[r, 0], dev(dx=to))
        take[r].start()
        sent.append(take[r])

    around = {}

    def along_y(k, rows, dy):
        d = remote(hbuf.at[c, 2, rows, :], hbuf.at[c, 2, rows, :], hs.at[2, k], hr.at[2, k], dev(dy=dy))
        d.start()
        around[k] = d
        sent.append(d)

    def rows_of(dy, half):
        return pl.ds(pl.multiple_of(((y + dy) % NY) * 64 + half * 32, 32), 32)

    def spread():
        take[2].wait_recv()
        along_y(1, rows_of(0, 0), 1)
        along_y(2, rows_of(0, 1), -1)
        along_y(3, rows_of(0, 1), 1)
        along_y(4, rows_of(0, 0), -1)

    def forward():
        around[1].wait_recv()
        along_y(5, rows_of(-1, 0), 1)
        around[2].wait_recv()
        along_y(6, rows_of(1, 1), -1)

    across = {}

    def share(r):
        if r == 2:
            for k in (3, 4, 5, 6):
                around[k].wait_recv()
        else:
            take[r].wait_recv()
        d = remote(hbuf.at[c, r], hbuf.at[c, r], hs.at[r, 7], hr.at[r, 7], dev(core=oc))
        d.start()
        across[r] = d
        sent.append(d)

    def product(r, core, add):
        def step(n, carry):
            at = pl.ds(pl.multiple_of(n * 256, 256), 256)
            res = jnp.dot(hbuf[core, r], wbuf[core, :, at], preferred_element_type=F32)
            pb[r, :, at] = pb[r, :, at] + res if add else res
            return carry

        lax.fori_loop(0, 4, step, 0)

    def arrived(r):
        across[r].wait_recv()

    RIGHT, LEFT = 1, -1
    ring = {}

    def send_x(k, dx):
        d = remote(sx.at[k], rx.at[k], xs.at[k], xr.at[k], dev(dx=dx))
        d.start()
        ring[k] = d
        sent.append(d)

    top, low = slice(0, 128), slice(128, 256)
    spread()
    direct(1)
    direct(3)
    for d in local:
        d.wait()
    product(0, 0, False)
    forward()
    product(0, 1, True)
    share(2)
    product(2, c, False)
    arrived(2)
    product(2, oc, True)
    pack_tall(pb[2, top, :], sx.at[0])
    send_x(0, RIGHT)
    pack_tall(pb[2, low, :], sx.at[1])
    send_x(1, LEFT)
    share(1)
    share(3)
    product(1, c, False)
    arrived(1)
    product(1, oc, True)
    pack_tall(pb[1, low, :], sx.at[2])
    send_x(2, RIGHT)
    product(3, c, False)
    arrived(3)
    product(3, oc, True)
    pack_tall(pb[3, top, :], sx.at[3])
    send_x(3, LEFT)
    ring[0].wait_recv()
    pack_tall(pb[1, top, :] + unpack_tall(rx.at[0], 128, 1024), sx.at[4])
    send_x(4, RIGHT)
    ring[1].wait_recv()
    pack_tall(pb[3, low, :] + unpack_tall(rx.at[1], 128, 1024), sx.at[5])
    send_x(5, LEFT)
    ring[2].wait_recv()
    pb[0, low, :] += unpack_tall(rx.at[2], 128, 1024)
    ring[3].wait_recv()
    pb[0, top, :] += unpack_tall(rx.at[3], 128, 1024)
    ring[4].wait_recv()
    pb[0, top, :] += unpack_tall(rx.at[4], 128, 1024)
    ring[5].wait_recv()
    pb[0, low, :] += unpack_tall(rx.at[5], 128, 1024)

    target = as_column(tgt[...].astype(F32))
    first = (v * 1024).astype(F32)
    lanes = lax.broadcasted_iota(jnp.int32, (128, 1024), 1).astype(F32) + first

    def send_e(k, src, dst, half, dx):
        d = remote(eb.at[src, half, :], eb.at[dst, half, :], gs.at[k], gr.at[k], dev(dx=dx))
        d.start()
        sent.append(d)
        return d

    upper, lower = pl.ds(0, 128), pl.ds(128, 128)
    tops, sums, picks = [], [], []
    for half in (top, low):
        logit = pb[0, half, :]
        m = jnp.max(logit, axis=1, keepdims=True)
        hot = lanes == target[half]
        picks.append(jnp.sum(jnp.where(hot, logit, 0.0), axis=1, keepdims=True))
        e = jnp.exp(logit - m)
        eb[0, half, :] = e.astype(BF16)
        pb[0, half, :] = e
        tops.append(m)
        sums.append(jnp.sum(e, axis=1, keepdims=True))
    a0 = send_e(0, 0, 3, upper, RIGHT)
    b0 = send_e(1, 0, 1, lower, LEFT)
    a1 = send_e(2, 0, 3, lower, RIGHT)
    b1 = send_e(3, 0, 1, upper, LEFT)
    st[0, 0, 0:1, :] = as_line(jnp.concatenate(tops, axis=0))
    st[0, 0, 1:2, :] = as_line(jnp.concatenate(sums, axis=0))
    st[0, 0, 2:3, :] = as_line(jnp.concatenate(picks, axis=0))

    def tell(level, places):
        out = []
        for k, p in enumerate(places, 1):
            d = remote(st.at[level, 0], st.at[level, k], ss.at[level, k], sr.at[level, k], p)
            d.start()
            sent.append(d)
            out.append(d)
        return out

    def join(level, told, out):
        for d in told:
            d.wait_recv()
        n = len(told) + 1
        m = st[level, 0, 0:1, :]
        for k in range(1, n):
            m = jnp.maximum(m, st[level, k, 0:1, :])
        s = jnp.zeros_like(m)
        q = jnp.zeros_like(m)
        for k in range(n):
            s = s + st[level, k, 1:2, :] * jnp.exp(st[level, k, 0:1, :] - m)
            q = q + st[level, k, 2:3, :]
        st[out, 0, 0:1, :] = m
        st[out, 0, 1:2, :] = s
        st[out, 0, 2:3, :] = q
        return m, s, q

    def turn(h):
        def step(n, carry):
            at = pl.ds(pl.multiple_of(n * 256, 256), 256)
            wt[h, :, at] = wbuf[h, at, :].T
            return carry

        lax.fori_loop(0, 4, step, 0)

    told = tell(0, [dev(core=oc)])
    join(0, told, 1)
    told = tell(1, [dev(dz=k) for k in range(1, NZ)])
    turn(0)
    join(1, told, 2)
    told = tell(2, [dev(dy=k) for k in (1, 2, 3)])
    turn(1)
    m, s, q = join(2, told, 3)
    loss[...] = m + jnp.log(s) - q
    weigh = cot[...]
    fx[0, 0:1, :] = weigh * (jnp.exp(st[0, 0, 0:1, :] - m) / s)
    fx[0, 1:2, :] = weigh * (jnp.exp(q - m) / s - 1.0)
    fx[0, 2:3, :] = tgt[...].astype(F32)
    line = {}
    for k in (1, 3, 2):
        r = 4 - k
        line[r] = remote(fx.at[0], fx.at[r], fs.at[r], fr.at[r], dev(dx=k))
        line[r].start()
        sent.append(line[r])

    def scale(r):
        if r:
            line[r].wait_recv()
        factor, at_target, target = (as_column(fx[r, i : i + 1, :]) for i in range(3))
        for half in (top, low):
            e = eb[r, half, :].astype(F32) if r else pb[0, half, :]
            g = jnp.where(lanes == target[half], at_target[half], e * factor[half])
            gall[r, half, :] = g.astype(BF16)

    pair, zd = {}, {}

    def block_product(*blocks):
        def step(n, carry):
            at = pl.ds(pl.multiple_of((n % 4) * 256, 256), 256)
            out = pl.ds(pl.multiple_of(n * 256, 256), 256)
            lhs = jnp.concatenate([gall[r] for r in blocks], axis=0)
            res = jnp.dot(lhs, wt[n // 4, :, at], preferred_element_type=F32)
            for i, r in enumerate(blocks):
                gt[r, :, :, :, out] = res[i * 256 : (i + 1) * 256].reshape(NZ, 2, 16, 256)
            return carry

        lax.fori_loop(0, 8, step, 0)
        for r in blocks:
            d = remote(gt.at[r, :, oc], rb.at[r], ds_.at[r], dr.at[r], dev(core=oc))
            d.start()
            pair[r] = d
            sent.append(d)

    def z_half(r, k, d, half):
        zz = (z + (4 - k if d == 0 else 4 + k)) % NZ
        cols = pl.ds(half * 1024, 1024)
        val = gt[r, zz, c, :, cols] + rb[r, zz, :, cols]
        if k > 1 or (k == 1 and half == d):
            zd[r, d, k - 1, half].wait_recv()
            val = val + unpack_flat(zr.at[r, d, k - 1, half], 16, 1024)
        if k == 4:
            return val
        pack_flat(val, zs.at[r, d, k, half])
        cp = remote(
            zs.at[r, d, k, half], zr.at[r, d, k, half],
            zss.at[r, d, k, half], zrs.at[r, d, k, half], dev(dz=1 if d == 0 else -1),
        )
        cp.start()
        zd[r, d, k, half] = cp
        sent.append(cp)

    def z_step(r, k):
        if k == 0:
            pair[r].wait_recv()
        if k < 4:
            for d in range(2):
                z_half(r, k, d, d)
        if k < 3:
            for d in range(2):
                z_half(r, k + 1, d, 1 - d)
        if k == 4:
            for half in (0, 1):
                other = zd[r, 1, 3, half]
                val = z_half(r, 4, 0, half)
                other.wait_recv()
                fin[r, :, half * 1024 : half * 1024 + 1024] = val + unpack_flat(zr.at[r, 1, 3, half], 16, 1024)

    def weight_tile(f):
        h, at = f // 4, pl.ds((f % 4) * 256, 256)
        lhs = hbuf[h, :, :, at].reshape(1024, 256)
        rhs = gall[...].reshape(1024, 1024)
        out = lax.dot_general(lhs, rhs, (((0,), (0,)), ((), ())), preferred_element_type=F32)
        gw[f * 256 : (f + 1) * 256, :] = out.astype(BF16)

    a0.wait_recv()
    f0 = send_e(4, 3, 2, upper, RIGHT)
    b0.wait_recv()
    f1 = send_e(5, 1, 2, lower, LEFT)
    scale(0)
    block_product(0)
    z_step(0, 0)
    a1.wait_recv()
    scale(3)
    b1.wait_recv()
    scale(1)
    block_product(3, 1)
    z_step(0, 1)
    f0.wait_recv()
    f1.wait_recv()
    scale(2)
    z_step(3, 0)
    block_product(2)
    z_step(1, 0)
    z_step(0, 2)
    z_step(2, 0)
    z_step(3, 1)
    z_step(1, 1)
    z_step(0, 3)
    z_step(2, 1)
    z_step(3, 2)
    z_step(1, 2)
    z_step(0, 4)
    z_step(2, 2)
    z_step(3, 3)
    z_step(1, 3)
    weight_tile(0)
    z_step(2, 3)
    z_step(3, 4)
    weight_tile(1)
    z_step(1, 4)
    weight_tile(2)
    weight_tile(3)
    z_step(2, 4)

    def held(k):
        return fin[(y + k - x + NX) % NX]

    home = []
    for k in (2, 1, 3):
        pack_flat(held(k), ys.at[k])
        d = remote(ys.at[k], yr.at[k], yss.at[k], yrs.at[k], dev(dy=k))
        d.start()
        sent.append(d)
        home.append((k, d))
    weight_tile(4)
    weight_tile(5)
    weight_tile(6)
    weight_tile(7)
    total = held(0)
    for k, d in home:
        d.wait_recv()
        total = total + unpack_flat(yr.at[k], 16, 2048)
    gh[...] = total.astype(BF16)

    def drain():
        for d in sent:
            d.wait_send()

    drain()


def finish(loss_in, gh_in, gw_in, loss, gh, gw, sem):
    pairs = ((gw_in, gw), (gh_in, gh), (loss_in, loss))
    copies = [pltpu.make_async_copy(a, b, sem.at[k]) for k, (a, b) in enumerate(pairs)]
    for d in copies:
        d.start()
    for d in copies:
        d.wait()


def shards(hidden, weight, targets, cotangent):
    vm, dma = pltpu.VMEM, pltpu.SemaphoreType.DMA
    space = pl.BlockSpec(memory_space=pltpu.VMEM)
    raw = pl.BlockSpec(memory_space=pl.ANY)
    loss, gh, gw = pl.pallas_call(
        kernel,
        out_shape=(
            jax.ShapeDtypeStruct((1, 256), F32),
            jax.ShapeDtypeStruct((16, 2048), BF16),
            jax.ShapeDtypeStruct((2048, 1024), BF16),
        ),
        in_specs=[pl.BlockSpec(memory_space=pltpu.HBM)] * 4,
        out_specs=(space, space, space),
        scratch_shapes=[
            vm((1, 256), jnp.int32),
            vm((1, 256), F32),
            vm((2, 4, 256, 1024), BF16),
            vm((2, 1024, 1024), BF16),
            vm((2, 1024, 1024), BF16),
            vm((4, 256, 1024), F32),
            vm((6, 1040, 128), I16),
            vm((6, 1040, 128), I16),
            vm((4, 8, 8, 256), F32),
            vm((4, 256, 1024), BF16),
            vm((4, 8, 256), F32),
            vm((4, 256, 1024), BF16),
            vm((4, NZ, 2, 16, 2048), F32),
            vm((4, NZ, 16, 2048), F32),
            vm((4, 2, 4, 2, 144, 128), I16),
            vm((4, 2, 4, 2, 144, 128), I16),
            vm((4, 16, 2048), F32),
            vm((4, 272, 128), I16),
            vm((4, 272, 128), I16),
            dma((6,)), dma((4, 8)), dma((4, 8)), dma((6,)), dma((6,)),
            dma((3, 8)), dma((3, 8)), dma((6,)), dma((6,)), dma((4,)), dma((4,)), dma((4,)), dma((4,)),
            dma((4, 2, 4, 2)), dma((4, 2, 4, 2)), dma((4,)), dma((4,)),
        ],
        compiler_params=pltpu.CompilerParams(
            collective_id=0, has_side_effects=True, vmem_limit_bytes=46 * 1024 * 1024
        ),
    )(hidden, weight, targets.reshape(1, 256), cotangent.reshape(1, 256))
    loss, gh, gw = pl.pallas_call(
        finish,
        out_shape=(
            jax.ShapeDtypeStruct((1, 256), F32),
            jax.ShapeDtypeStruct((16, 2048), BF16),
            jax.ShapeDtypeStruct((2048, 1024), BF16),
        ),
        in_specs=[space, space, space],
        out_specs=(raw, raw, raw),
        scratch_shapes=[dma((3,))],
        compiler_params=pltpu.CompilerParams(vmem_limit_bytes=8 * 1024 * 1024),
    )(loss, gh, gw)
    return loss.reshape(256), gh, gw


def solution(mesh):
    in_specs = (P("dp", None), P("dp", "vocab"), P("dp"), P("dp"))
    out_specs = (P("dp"), P("vocab", "dp"), P("dp", "vocab"))
    return jax.shard_map(shards, mesh=mesh, in_specs=in_specs, out_specs=out_specs, check_vma=False)
```

```python
import jax
import jax.numpy as jnp
from jax import lax
from jax.experimental import pallas as pl
from jax.experimental.pallas import tpu as pltpu
from jax.sharding import PartitionSpec as P

F32, BF16, I16 = jnp.float32, jnp.bfloat16, jnp.int16
NX, NY, NZ = 4, 4, 8
FINE = 64.0 / 0.6931471805599453
TOP = 32700.0


def row_code(x):
    top = jnp.max(jnp.abs(x), axis=1, keepdims=True)
    return jnp.ceil(jnp.log(jnp.maximum(top, 1e-30)) * FINE)


def pack_tall(x, dst):
    rows, cols = x.shape
    k = row_code(x)
    inv = jnp.exp(k * (-1.0 / FINE)) * TOP
    for j in range(cols // 128):
        dst[j * rows : (j + 1) * rows, :] = jnp.round(x[:, j * 128 : (j + 1) * 128] * inv).astype(I16)
    line = jnp.broadcast_to(k, (rows, 128)).T[0:1, :]
    dst[cols // 128 * rows : cols // 128 * rows + 16, :] = jnp.broadcast_to(line, (16, 128)).astype(I16)


def unpack_tall(src, rows, cols):
    at = cols // 128 * rows
    line = src[at : at + 16, :].astype(F32)[0:1, :]
    k = jnp.broadcast_to(line, (rows, rows)).T
    scale = jnp.exp(k * (1.0 / FINE)) * (1.0 / TOP)
    return jnp.concatenate(
        [src[j * rows : (j + 1) * rows, :].astype(F32) * scale for j in range(cols // 128)], axis=1
    )


def pack_flat(x, dst):
    rows, cols = x.shape
    k = row_code(x)
    inv = jnp.exp(k * (-1.0 / FINE)) * TOP
    for j in range(cols // 128):
        dst[j * rows : (j + 1) * rows, :] = jnp.round(x[:, j * 128 : (j + 1) * 128] * inv).astype(I16)
    dst[cols // 128 * rows : (cols // 128 + 1) * rows, :] = jnp.broadcast_to(k, (rows, 128)).astype(I16)


def unpack_flat(src, rows, cols):
    at = cols // 128 * rows
    scale = jnp.exp(src[at : at + rows, :].astype(F32) * (1.0 / FINE)) * (1.0 / TOP)
    return jnp.concatenate(
        [src[j * rows : (j + 1) * rows, :].astype(F32) * scale for j in range(cols // 128)], axis=1
    )


def as_column(line):
    n = line.shape[1]
    return jnp.broadcast_to(line, (128, n)).T[:, 0:1]


def as_line(column):
    n = column.shape[0]
    return jnp.broadcast_to(column, (n, 128)).T[0:1, :]


def kernel(
    hid, w, tgt_in, cot_in, loss, gh, gw,
    tgt, cot,    hbuf, wbuf, wt, pb, sx, rx, st, eb, fx, gall, hot0, vt, gt, rb, zs, zr, fin, ys, yr,
    lsem, hs, hr, xs, xr, ss, sr, gs, gr, fs, fr, ds_, dr, zss, zrs, yss, yrs,
):
    x = lax.axis_index("dp")
    v = lax.axis_index("vocab")
    y, z, c = v // (2 * NZ), (v // 2) % NZ, v % 2
    oc = 1 - c

    def dev(dx=0, dy=0, dz=0, core=None):
        yy, zz = (y + dy) % NY, (z + dz) % NZ
        cc = c if core is None else core
        return {"dp": (x + dx) % NX, "vocab": (yy * NZ + zz) * 2 + cc}

    def remote(src, dst, send, recv, to):
        return pltpu.make_async_remote_copy(
            src_ref=src, dst_ref=dst, send_sem=send, recv_sem=recv,
            device_id=to, device_id_type=pl.DeviceIdType.MESH,
        )

    local = [pltpu.make_async_copy(w.at[pl.ds(h * 1024, 1024), :], wbuf.at[h], lsem.at[h]) for h in range(2)]
    for h in range(2):
        cols = pl.multiple_of(x * 2048 + h * 1024, 1024)
        local.append(pltpu.make_async_copy(hid.at[:, pl.ds(cols, 1024)], hbuf.at[h, 0], lsem.at[2 + h]))
    local.append(pltpu.make_async_copy(tgt_in, tgt, lsem.at[4]))
    local.append(pltpu.make_async_copy(cot_in, cot, lsem.at[5]))
    for d in local:
        d.start()

    barrier = pltpu.get_barrier_semaphore()
    peers = [dev(dx=k) for k in (1, 2, 3)] + [dev(core=oc)]
    peers += [dev(dy=k, core=cc) for k in (1, 2, 3) for cc in (c, oc)] + [dev(dz=k) for k in range(1, NZ)]
    for p in peers:
        pl.semaphore_signal(barrier, inc=1, device_id=p, device_id_type=pl.DeviceIdType.MESH)
    pl.semaphore_wait(barrier, len(peers))

    sent = []
    mine = pl.ds(pl.multiple_of(y * 64, 64), 64)
    take = {}
    def columns_for(r):
        to = (4 - r) % 4
        return to, pl.ds(pl.multiple_of(((x + to) % NX) * 2048 + c * 1024, 1024), 1024)

    to, cols = columns_for(2)
    take[2] = remote(hid.at[mine, cols], hbuf.at[c, 2, mine, :], hs.at[0], hr.at[0], dev(dx=to))
    take[2].start()
    sent.append(take[2])

    def direct(r):
        to, cols = columns_for(r)
        take[r] = remote(hid.at[:, cols], hbuf.at[c, r], hs.at[r], hr.at[r], dev(dx=to))
        take[r].start()
        sent.append(take[r])

    around = {}

    def along_y(k, rows, dy):
        d = remote(hbuf.at[c, 2, rows, :], hbuf.at[c, 2, rows, :], hs.at[3 + k], hr.at[3 + k], dev(dy=dy))
        d.start()
        around[k] = d
        sent.append(d)

    def rows_of(dy, half):
        return pl.ds(pl.multiple_of(((y + dy) % NY) * 64 + half * 32, 32), 32)

    def spread():
        take[2].wait_recv()
        along_y(1, rows_of(0, 0), 1)
        along_y(2, rows_of(0, 1), -1)
        along_y(3, rows_of(0, 1), 1)
        along_y(4, rows_of(0, 0), -1)

    def forward():
        around[1].wait_recv()
        along_y(5, rows_of(-1, 0), 1)
        around[2].wait_recv()
        along_y(6, rows_of(1, 1), -1)

    across = {}

    def share(r):
        if r == 2:
            for k in (3, 4, 5, 6):
                around[k].wait_recv()
        else:
            take[r].wait_recv()
        d = remote(hbuf.at[c, r], hbuf.at[c, r], hs.at[9 + r], hr.at[9 + r], dev(core=oc))
        d.start()
        across[r] = d
        sent.append(d)

    def product(r, core, add):
        def step(n, carry):
            at = pl.ds(pl.multiple_of(n * 256, 256), 256)
            res = jnp.dot(hbuf[core, r], wbuf[core, :, at], preferred_element_type=F32)
            pb[r, :, at] = pb[r, :, at] + res if add else res
            return carry

        lax.fori_loop(0, 4, step, 0)

    def arrived(r):
        across[r].wait_recv()

    def turn(h):
        def step(n, carry):
            at = pl.ds(pl.multiple_of(n * 256, 256), 256)
            wt[h, :, at] = wbuf[h, at, :].T
            return carry

        lax.fori_loop(0, 4, step, 0)

    RIGHT, LEFT = 1, -1
    ring = {}

    def send_x(k, dx):
        d = remote(sx.at[k], rx.at[k], xs.at[k], xr.at[k], dev(dx=dx))
        d.start()
        ring[k] = d
        sent.append(d)

    top, low = slice(0, 128), slice(128, 256)
    spread()
    direct(1)
    direct(3)
    for d in local:
        d.wait()
    product(0, 0, False)
    forward()
    product(0, 1, True)
    share(2)
    product(2, c, False)
    arrived(2)
    product(2, oc, True)
    pack_tall(pb[2, top, :], sx.at[0])
    send_x(0, RIGHT)
    pack_tall(pb[2, low, :], sx.at[1])
    send_x(1, LEFT)
    share(1)
    share(3)
    product(1, c, False)
    arrived(1)
    product(1, oc, True)
    pack_tall(pb[1, low, :], sx.at[2])
    send_x(2, RIGHT)
    product(3, c, False)
    arrived(3)
    product(3, oc, True)
    pack_tall(pb[3, top, :], sx.at[3])
    send_x(3, LEFT)
    ring[0].wait_recv()
    pack_tall(pb[1, top, :] + unpack_tall(rx.at[0], 128, 1024), sx.at[4])
    send_x(4, RIGHT)
    ring[1].wait_recv()
    pack_tall(pb[3, low, :] + unpack_tall(rx.at[1], 128, 1024), sx.at[5])
    send_x(5, LEFT)
    turn(0)
    turn(1)
    ring[2].wait_recv()
    pb[0, low, :] += unpack_tall(rx.at[2], 128, 1024)
    ring[3].wait_recv()
    pb[0, top, :] += unpack_tall(rx.at[3], 128, 1024)
    ring[4].wait_recv()
    pb[0, top, :] += unpack_tall(rx.at[4], 128, 1024)
    ring[5].wait_recv()
    pb[0, low, :] += unpack_tall(rx.at[5], 128, 1024)

    target = as_column(tgt[...].astype(F32))
    first = (v * 1024).astype(F32)
    lanes = lax.broadcasted_iota(jnp.int32, (128, 1024), 1).astype(F32) + first

    def send_e(k, src, dst, half, dx):
        d = remote(eb.at[src, half, :], eb.at[dst, half, :], gs.at[k], gr.at[k], dev(dx=dx))
        d.start()
        sent.append(d)
        return d

    upper, lower = pl.ds(0, 128), pl.ds(128, 128)
    tops, sums, picks = [], [], []
    for half in (top, low):
        logit = pb[0, half, :]
        m = jnp.max(logit, axis=1, keepdims=True)
        hot = lanes == target[half]
        picks.append(jnp.sum(jnp.where(hot, logit, 0.0), axis=1, keepdims=True))
        e = jnp.exp(logit - m)
        eb[0, half, :] = e.astype(BF16)
        gall[0, half, :] = jnp.where(hot, 0.0, e).astype(BF16)
        hot0[half, :] = hot.astype(F32).astype(BF16)
        pb[0, half, :] = e
        tops.append(m)
        sums.append(jnp.sum(e, axis=1, keepdims=True))
    a0 = send_e(0, 0, 3, upper, RIGHT)
    b0 = send_e(1, 0, 1, lower, LEFT)
    a1 = send_e(2, 0, 3, lower, RIGHT)
    b1 = send_e(3, 0, 1, upper, LEFT)
    st[0, 0, 0:1, :] = as_line(jnp.concatenate(tops, axis=0))
    st[0, 0, 1:2, :] = as_line(jnp.concatenate(sums, axis=0))
    st[0, 0, 2:3, :] = as_line(jnp.concatenate(picks, axis=0))

    def tell(level, places):
        out = []
        for k, p in enumerate(places, 1):
            d = remote(st.at[level, 0], st.at[level, k], ss.at[level, k], sr.at[level, k], p)
            d.start()
            sent.append(d)
            out.append(d)
        return out

    def join(level, told, out):
        for d in told:
            d.wait_recv()
        n = len(told) + 1
        m = st[level, 0, 0:1, :]
        for k in range(1, n):
            m = jnp.maximum(m, st[level, k, 0:1, :])
        s = jnp.zeros_like(m)
        q = jnp.zeros_like(m)
        for k in range(n):
            s = s + st[level, k, 1:2, :] * jnp.exp(st[level, k, 0:1, :] - m)
            q = q + st[level, k, 2:3, :]
        st[out, 0, 0:1, :] = m
        st[out, 0, 1:2, :] = s
        st[out, 0, 2:3, :] = q
        return m, s, q

    def row_product(lhs, out):
        def step(n, carry):
            at = pl.ds(pl.multiple_of((n % 4) * 256, 256), 256)
            to = pl.ds(pl.multiple_of(n * 256, 256), 256)
            res = jnp.dot(lhs[...], wt[n // 4, :, at], preferred_element_type=F32)
            out[:, :, :, to] = res.reshape(NZ, 2, 16, 256)
            return carry

        lax.fori_loop(0, 8, step, 0)

    told = tell(0, [dev(core=oc)] + [dev(dy=k, core=cc) for k in (1, 2, 3) for cc in (c, oc)])
    row_product(hot0, vt)
    join(0, told, 1)
    told = tell(1, [dev(dz=k) for k in range(1, NZ)])
    row_product(gall.at[0], gt.at[0])
    m, s, q = join(1, told, 2)
    loss[...] = m + jnp.log(s) - q
    weigh = cot[...]
    fx[0, 0:1, :] = weigh * (jnp.exp(st[0, 0, 0:1, :] - m) / s)
    fx[0, 1:2, :] = (weigh * (jnp.exp(q - m) / s - 1.0)).astype(BF16).astype(F32)
    fx[0, 2:3, :] = tgt[...].astype(F32)
    line = {}
    for k in (1, 3, 2):
        r = 4 - k
        line[r] = remote(fx.at[0], fx.at[r], fs.at[r], fr.at[r], dev(dx=k))
        line[r].start()
        sent.append(line[r])

    def scale(r):
        if r:
            line[r].wait_recv()
        factor, at_target, target = (as_column(fx[r, i : i + 1, :]) for i in range(3))
        for half in (top, low):
            e = eb[r, half, :].astype(F32) if r else pb[0, half, :]
            g = jnp.where(lanes == target[half], at_target[half], e * factor[half])
            gall[r, half, :] = g.astype(BF16)

    pair, zd = {}, {}

    def send_pair(r, h):
        cols = pl.ds(h * 1024, 1024)
        d = remote(gt.at[r, :, oc, :, cols], rb.at[r, :, :, cols], ds_.at[r, h], dr.at[r, h], dev(core=oc))
        d.start()
        pair[r, h] = d
        sent.append(d)

    def block_product(h, *blocks):
        def step(n, carry):
            at = pl.ds(pl.multiple_of(n * 256, 256), 256)
            out = pl.ds(pl.multiple_of(n * 256 + h * 1024, 256), 256)
            lhs = jnp.concatenate([gall[r] for r in blocks], axis=0)
            res = jnp.dot(lhs, wt[h, :, at], preferred_element_type=F32)
            for i, r in enumerate(blocks):
                gt[r, :, :, :, out] = res[i * 256 : (i + 1) * 256].reshape(NZ, 2, 16, 256)
            return carry

        lax.fori_loop(0, 4, step, 0)
        for r in blocks:
            send_pair(r, h)

    def own_block(h):
        factor, at_target = (as_column(fx[0, i : i + 1, :]).reshape(NZ, 2, 16, 1) for i in range(2))
        for j in range(h * 4, h * 4 + 4):
            cols = slice(j * 256, j * 256 + 256)
            gt[0, :, :, :, cols] = gt[0, :, :, :, cols] * factor + vt[:, :, :, cols] * at_target
        send_pair(0, h)

    def z_half(r, k, d, half):
        zz = (z + (4 - k if d == 0 else 4 + k)) % NZ
        cols = pl.ds(half * 1024, 1024)
        val = gt[r, zz, c, :, cols] + rb[r, zz, :, cols]
        if k > 1 or (k == 1 and half == d):
            zd[r, d, k - 1, half].wait_recv()
            val = val + unpack_flat(zr.at[r, d, k - 1, half], 16, 1024)
        if k == 4:
            return val
        pack_flat(val, zs.at[r, d, k, half])
        cp = remote(
            zs.at[r, d, k, half], zr.at[r, d, k, half],
            zss.at[r, d, k, half], zrs.at[r, d, k, half], dev(dz=1 if d == 0 else -1),
        )
        cp.start()
        zd[r, d, k, half] = cp
        sent.append(cp)

    def z_step(r, k):
        if k < 4:
            for d in range(2):
                if k == 0:
                    pair[r, d].wait_recv()
                z_half(r, k, d, d)
        if k < 3:
            for d in range(2):
                z_half(r, k + 1, d, 1 - d)
        if k == 4:
            for half in (0, 1):
                other = zd[r, 1, 3, half]
                val = z_half(r, 4, 0, half)
                other.wait_recv()
                fin[r, :, half * 1024 : half * 1024 + 1024] = val + unpack_flat(zr.at[r, 1, 3, half], 16, 1024)

    def weight_tile(f):
        h, at = f // 4, pl.ds((f % 4) * 256, 256)
        lhs = hbuf[h, :, :, at].reshape(1024, 256)
        rhs = gall[...].reshape(1024, 1024)
        out = lax.dot_general(lhs, rhs, (((0,), (0,)), ((), ())), preferred_element_type=F32)
        gw[f * 256 : (f + 1) * 256, :] = out.astype(BF16)

    a0.wait_recv()
    f0 = send_e(4, 3, 2, upper, RIGHT)
    b0.wait_recv()
    f1 = send_e(5, 1, 2, lower, LEFT)
    own_block(0)
    own_block(1)
    scale(0)
    z_step(0, 0)
    a1.wait_recv()
    scale(3)
    b1.wait_recv()
    scale(1)
    block_product(0, 3, 1)
    z_step(0, 1)
    block_product(1, 3, 1)
    f0.wait_recv()
    f1.wait_recv()
    scale(2)
    block_product(0, 2)
    z_step(0, 2)
    z_step(3, 0)
    z_step(1, 0)
    block_product(1, 2)
    z_step(2, 0)
    z_step(0, 3)
    z_step(3, 1)
    z_step(1, 1)
    z_step(0, 4)
    weight_tile(0)
    z_step(2, 1)
    weight_tile(1)
    z_step(3, 2)
    weight_tile(2)
    z_step(1, 2)
    weight_tile(3)
    z_step(2, 2)
    z_step(3, 3)
    weight_tile(4)
    z_step(1, 3)
    z_step(2, 3)
    weight_tile(5)
    z_step(3, 4)
    z_step(1, 4)
    z_step(2, 4)

    def held(k):
        return fin[(y + k - x + NX) % NX]

    home = []
    for k in (2, 1, 3):
        pack_flat(held(k), ys.at[k])
        d = remote(ys.at[k], yr.at[k], yss.at[k], yrs.at[k], dev(dy=k))
        d.start()
        sent.append(d)
        home.append((k, d))
    weight_tile(6)
    weight_tile(7)
    total = held(0)
    for k, d in home:
        d.wait_recv()
        total = total + unpack_flat(yr.at[k], 16, 2048)
    gh[...] = total.astype(BF16)

    def drain():
        for d in sent:
            d.wait_send()

    drain()


def finish(loss_in, gh_in, gw_in, loss, gh, gw, sem):
    pairs = ((gw_in, gw), (gh_in, gh), (loss_in, loss))
    copies = [pltpu.make_async_copy(a, b, sem.at[k]) for k, (a, b) in enumerate(pairs)]
    for d in copies:
        d.start()
    for d in copies:
        d.wait()


def shards(hidden, weight, targets, cotangent):
    args = (hidden, weight, targets.reshape(1, 256), cotangent.reshape(1, 256))
    vm, dma = pltpu.VMEM, pltpu.SemaphoreType.DMA
    space = pl.BlockSpec(memory_space=pltpu.VMEM)
    raw = pl.BlockSpec(memory_space=pl.ANY)
    loss, gh, gw = pl.pallas_call(
        kernel,
        out_shape=(
            jax.ShapeDtypeStruct((1, 256), F32),
            jax.ShapeDtypeStruct((16, 2048), BF16),
            jax.ShapeDtypeStruct((2048, 1024), BF16),
        ),
        in_specs=[pl.BlockSpec(memory_space=pltpu.HBM)] * 4,
        out_specs=(space, space, space),
        scratch_shapes=[
            vm((1, 256), jnp.int32),
            vm((1, 256), F32),
            vm((2, 4, 256, 1024), BF16),
            vm((2, 1024, 1024), BF16),
            vm((2, 1024, 1024), BF16),
            vm((4, 256, 1024), F32),
            vm((6, 1040, 128), I16),
            vm((6, 1040, 128), I16),
            vm((4, 8, 8, 256), F32),
            vm((4, 256, 1024), BF16),
            vm((4, 8, 256), F32),
            vm((4, 256, 1024), BF16),
            vm((256, 1024), BF16),
            vm((NZ, 2, 16, 2048), F32),
            vm((4, NZ, 2, 16, 2048), F32),
            vm((4, NZ, 16, 2048), F32),
            vm((4, 2, 4, 2, 144, 128), I16),
            vm((4, 2, 4, 2, 144, 128), I16),
            vm((4, 16, 2048), F32),
            vm((4, 272, 128), I16),
            vm((4, 272, 128), I16),
            dma((6,)), dma((13,)), dma((13,)), dma((6,)), dma((6,)),
            dma((2, 8)), dma((2, 8)), dma((6,)), dma((6,)), dma((4,)), dma((4,)), dma((4, 2)), dma((4, 2)),
            dma((4, 2, 4, 2)), dma((4, 2, 4, 2)), dma((4,)), dma((4,)),
        ],
        compiler_params=pltpu.CompilerParams(
            collective_id=0, has_side_effects=True, vmem_limit_bytes=49 * 1024 * 1024
        ),
    )(*(pltpu.with_memory_space_constraint(a, pltpu.HBM) for a in args))
    loss, gh, gw = pl.pallas_call(
        finish,
        out_shape=(
            jax.ShapeDtypeStruct((1, 256), F32),
            jax.ShapeDtypeStruct((16, 2048), BF16),
            jax.ShapeDtypeStruct((2048, 1024), BF16),
        ),
        in_specs=[space, space, space],
        out_specs=(raw, raw, raw),
        scratch_shapes=[dma((3,))],
        compiler_params=pltpu.CompilerParams(vmem_limit_bytes=8 * 1024 * 1024),
    )(loss, gh, gw)
    return loss.reshape(256), gh, gw


def solution(mesh):
    in_specs = (P("dp", None), P("dp", "vocab"), P("dp"), P("dp"))
    out_specs = (P("dp"), P("vocab", "dp"), P("dp", "vocab"))
    return jax.shard_map(shards, mesh=mesh, in_specs=in_specs, out_specs=out_specs, check_vma=False)
```

```python
import jax
import jax.numpy as jnp
from jax import lax
from jax.experimental import pallas as pl
from jax.experimental.pallas import tpu as pltpu
from jax.sharding import PartitionSpec as P

F32, BF16, I16 = jnp.float32, jnp.bfloat16, jnp.int16
NX, NY, NZ = 4, 4, 8
FINE = 64.0 / 0.6931471805599453
TOP = 32700.0


def row_code(x):
    top = jnp.max(jnp.abs(x), axis=1, keepdims=True)
    return jnp.ceil(jnp.log(jnp.maximum(top, 1e-30)) * FINE)


def pack_tall(x, dst):
    rows, cols = x.shape
    k = row_code(x)
    inv = jnp.exp(k * (-1.0 / FINE)) * TOP
    for j in range(cols // 128):
        dst[j * rows : (j + 1) * rows, :] = jnp.round(x[:, j * 128 : (j + 1) * 128] * inv).astype(I16)
    line = jnp.broadcast_to(k, (rows, 128)).T[0:1, :]
    dst[cols // 128 * rows : cols // 128 * rows + 16, :] = jnp.broadcast_to(line, (16, 128)).astype(I16)


def unpack_tall(src, rows, cols):
    at = cols // 128 * rows
    line = src[at : at + 16, :].astype(F32)[0:1, :]
    k = jnp.broadcast_to(line, (rows, rows)).T
    scale = jnp.exp(k * (1.0 / FINE)) * (1.0 / TOP)
    return jnp.concatenate(
        [src[j * rows : (j + 1) * rows, :].astype(F32) * scale for j in range(cols // 128)], axis=1
    )


def pack_flat(x, dst):
    rows, cols = x.shape
    k = row_code(x)
    inv = jnp.exp(k * (-1.0 / FINE)) * TOP
    for j in range(cols // 128):
        dst[j * rows : (j + 1) * rows, :] = jnp.round(x[:, j * 128 : (j + 1) * 128] * inv).astype(I16)
    dst[cols // 128 * rows : (cols // 128 + 1) * rows, :] = jnp.broadcast_to(k, (rows, 128)).astype(I16)


def unpack_flat(src, rows, cols):
    at = cols // 128 * rows
    scale = jnp.exp(src[at : at + rows, :].astype(F32) * (1.0 / FINE)) * (1.0 / TOP)
    return jnp.concatenate(
        [src[j * rows : (j + 1) * rows, :].astype(F32) * scale for j in range(cols // 128)], axis=1
    )


def as_column(line):
    n = line.shape[1]
    return jnp.broadcast_to(line, (128, n)).T[:, 0:1]


def as_line(column):
    n = column.shape[0]
    return jnp.broadcast_to(column, (n, 128)).T[0:1, :]


def kernel(
    hid, w, tgt_in, cot_in, loss, gh, gw,
    tgt, cot, xh,     hbuf, wbuf, wt, pb, sx, rx, st, eb, fx, gall, hot0, vt, gt, rb, zs, zr, fin, ys, yr,
    lsem, hs, hr, xs, xr, ss, sr, gs, gr, fs, fr, ds_, dr, zss, zrs, yss, yrs,
):
    x = lax.axis_index("dp")
    v = lax.axis_index("vocab")
    y, z, c = v // (2 * NZ), (v // 2) % NZ, v % 2
    oc = 1 - c

    def dev(dx=0, dy=0, dz=0, core=None):
        yy, zz = (y + dy) % NY, (z + dz) % NZ
        cc = c if core is None else core
        return {"dp": (x + dx) % NX, "vocab": (yy * NZ + zz) * 2 + cc}

    def remote(src, dst, send, recv, to):
        return pltpu.make_async_remote_copy(
            src_ref=src, dst_ref=dst, send_sem=send, recv_sem=recv,
            device_id=to, device_id_type=pl.DeviceIdType.MESH,
        )

    def columns_for(r):
        to = (4 - r) % 4
        return to, pl.ds(pl.multiple_of(((x + to) % NX) * 2048 + c * 1024, 1024), 1024)

    mine = pl.ds(pl.multiple_of(y * 64, 64), 64)
    far_to, far_cols = columns_for(2)
    ahead = pltpu.make_async_copy(hid.at[mine, far_cols], xh, lsem.at[6])
    ahead.start()

    local = [pltpu.make_async_copy(w.at[pl.ds(h * 1024, 1024), :], wbuf.at[h], lsem.at[h]) for h in range(2)]
    for h in range(2):
        cols = pl.multiple_of(x * 2048 + h * 1024, 1024)
        local.append(pltpu.make_async_copy(hid.at[:, pl.ds(cols, 1024)], hbuf.at[h, 0], lsem.at[2 + h]))
    local.append(pltpu.make_async_copy(tgt_in, tgt, lsem.at[4]))
    local.append(pltpu.make_async_copy(cot_in, cot, lsem.at[5]))
    for d in local:
        d.start()

    barrier = pltpu.get_barrier_semaphore()
    peers = [dev(dx=k) for k in (1, 2, 3)] + [dev(core=oc)]
    peers += [dev(dy=k, core=cc) for k in (1, 2, 3) for cc in (c, oc)] + [dev(dz=k) for k in range(1, NZ)]
    for p in peers:
        pl.semaphore_signal(barrier, inc=1, device_id=p, device_id_type=pl.DeviceIdType.MESH)
    pl.semaphore_wait(barrier, len(peers))

    sent = []
    take = {}
    ahead.wait()
    take[2] = remote(xh, hbuf.at[c, 2, mine, :], hs.at[0], hr.at[0], dev(dx=far_to))
    take[2].start()
    sent.append(take[2])

    def direct(r):
        to, cols = columns_for(r)
        take[r] = remote(hid.at[:, cols], hbuf.at[c, r], hs.at[r], hr.at[r], dev(dx=to))
        take[r].start()
        sent.append(take[r])

    around = {}

    def along_y(k, rows, dy):
        d = remote(hbuf.at[c, 2, rows, :], hbuf.at[c, 2, rows, :], hs.at[3 + k], hr.at[3 + k], dev(dy=dy))
        d.start()
        around[k] = d
        sent.append(d)

    def rows_of(dy, half):
        return pl.ds(pl.multiple_of(((y + dy) % NY) * 64 + half * 32, 32), 32)

    def spread():
        take[2].wait_recv()
        along_y(1, rows_of(0, 0), 1)
        along_y(2, rows_of(0, 1), -1)
        along_y(3, rows_of(0, 1), 1)
        along_y(4, rows_of(0, 0), -1)

    def forward():
        around[1].wait_recv()
        along_y(5, rows_of(-1, 0), 1)
        around[2].wait_recv()
        along_y(6, rows_of(1, 1), -1)

    across = {}

    def share(r):
        if r == 2:
            for k in (3, 4, 5, 6):
                around[k].wait_recv()
        else:
            take[r].wait_recv()
        d = remote(hbuf.at[c, r], hbuf.at[c, r], hs.at[9 + r], hr.at[9 + r], dev(core=oc))
        d.start()
        across[r] = d
        sent.append(d)

    def product(r, core, add):
        def step(n, carry):
            at = pl.ds(pl.multiple_of(n * 256, 256), 256)
            res = jnp.dot(hbuf[core, r], wbuf[core, :, at], preferred_element_type=F32)
            pb[r, :, at] = pb[r, :, at] + res if add else res
            return carry

        lax.fori_loop(0, 4, step, 0)

    def arrived(r):
        across[r].wait_recv()

    def turn(h):
        def step(n, carry):
            at = pl.ds(pl.multiple_of(n * 256, 256), 256)
            wt[h, :, at] = wbuf[h, at, :].T
            return carry

        lax.fori_loop(0, 4, step, 0)

    RIGHT, LEFT = 1, -1
    ring = {}

    def send_x(k, dx):
        d = remote(sx.at[k], rx.at[k], xs.at[k], xr.at[k], dev(dx=dx))
        d.start()
        ring[k] = d
        sent.append(d)

    top, low = slice(0, 128), slice(128, 256)
    spread()
    direct(1)
    direct(3)
    for d in local:
        d.wait()
    product(0, 0, False)
    forward()
    product(0, 1, True)
    share(2)
    product(2, c, False)
    arrived(2)
    product(2, oc, True)
    pack_tall(pb[2, top, :], sx.at[0])
    send_x(0, RIGHT)
    pack_tall(pb[2, low, :], sx.at[1])
    send_x(1, LEFT)
    share(1)
    share(3)
    product(1, c, False)
    arrived(1)
    product(1, oc, True)
    pack_tall(pb[1, low, :], sx.at[2])
    send_x(2, RIGHT)
    product(3, c, False)
    arrived(3)
    product(3, oc, True)
    pack_tall(pb[3, top, :], sx.at[3])
    send_x(3, LEFT)
    ring[0].wait_recv()
    pack_tall(pb[1, top, :] + unpack_tall(rx.at[0], 128, 1024), sx.at[4])
    send_x(4, RIGHT)
    ring[1].wait_recv()
    pack_tall(pb[3, low, :] + unpack_tall(rx.at[1], 128, 1024), sx.at[5])
    send_x(5, LEFT)
    turn(0)
    turn(1)
    ring[2].wait_recv()
    pb[0, low, :] += unpack_tall(rx.at[2], 128, 1024)
    ring[3].wait_recv()
    pb[0, top, :] += unpack_tall(rx.at[3], 128, 1024)
    ring[4].wait_recv()
    pb[0, top, :] += unpack_tall(rx.at[4], 128, 1024)
    ring[5].wait_recv()
    pb[0, low, :] += unpack_tall(rx.at[5], 128, 1024)

    target = as_column(tgt[...].astype(F32))
    first = (v * 1024).astype(F32)
    lanes = lax.broadcasted_iota(jnp.int32, (128, 1024), 1).astype(F32) + first

    def send_e(k, src, dst, half, dx):
        d = remote(eb.at[src, half, :], eb.at[dst, half, :], gs.at[k], gr.at[k], dev(dx=dx))
        d.start()
        sent.append(d)
        return d

    upper, lower = pl.ds(0, 128), pl.ds(128, 128)
    tops, sums, picks = [], [], []
    for half in (top, low):
        logit = pb[0, half, :]
        m = jnp.max(logit, axis=1, keepdims=True)
        hot = lanes == target[half]
        picks.append(jnp.sum(jnp.where(hot, logit, 0.0), axis=1, keepdims=True))
        e = jnp.exp(logit - m)
        eb[0, half, :] = e.astype(BF16)
        gall[0, half, :] = jnp.where(hot, 0.0, e).astype(BF16)
        hot0[half, :] = hot.astype(F32).astype(BF16)
        pb[0, half, :] = e
        tops.append(m)
        sums.append(jnp.sum(e, axis=1, keepdims=True))
    a0 = send_e(0, 0, 3, upper, RIGHT)
    b0 = send_e(1, 0, 1, lower, LEFT)
    a1 = send_e(2, 0, 3, lower, RIGHT)
    b1 = send_e(3, 0, 1, upper, LEFT)
    st[0, 0, 0:1, :] = as_line(jnp.concatenate(tops, axis=0))
    st[0, 0, 1:2, :] = as_line(jnp.concatenate(sums, axis=0))
    st[0, 0, 2:3, :] = as_line(jnp.concatenate(picks, axis=0))

    def tell(level, places):
        out = []
        for k, p in enumerate(places, 1):
            d = remote(st.at[level, 0], st.at[level, k], ss.at[level, k], sr.at[level, k], p)
            d.start()
            sent.append(d)
            out.append(d)
        return out

    def join(level, told, out):
        for d in told:
            d.wait_recv()
        n = len(told) + 1
        m = st[level, 0, 0:1, :]
        for k in range(1, n):
            m = jnp.maximum(m, st[level, k, 0:1, :])
        s = jnp.zeros_like(m)
        q = jnp.zeros_like(m)
        for k in range(n):
            s = s + st[level, k, 1:2, :] * jnp.exp(st[level, k, 0:1, :] - m)
            q = q + st[level, k, 2:3, :]
        st[out, 0, 0:1, :] = m
        st[out, 0, 1:2, :] = s
        st[out, 0, 2:3, :] = q
        return m, s, q

    def row_product(lhs, out):
        def step(n, carry):
            at = pl.ds(pl.multiple_of((n % 4) * 256, 256), 256)
            to = pl.ds(pl.multiple_of(n * 256, 256), 256)
            res = jnp.dot(lhs[...], wt[n // 4, :, at], preferred_element_type=F32)
            out[:, :, :, to] = res.reshape(NZ, 2, 16, 256)
            return carry

        lax.fori_loop(0, 8, step, 0)

    told = tell(0, [dev(core=oc)] + [dev(dy=k, core=cc) for k in (1, 2, 3) for cc in (c, oc)])
    row_product(hot0, vt)
    join(0, told, 1)
    told = tell(1, [dev(dz=k) for k in range(1, NZ)])
    row_product(gall.at[0], gt.at[0])
    m, s, q = join(1, told, 2)
    loss[...] = m + jnp.log(s) - q
    weigh = cot[...]
    fx[0, 0:1, :] = weigh * (jnp.exp(st[0, 0, 0:1, :] - m) / s)
    fx[0, 1:2, :] = (weigh * (jnp.exp(q - m) / s - 1.0)).astype(BF16).astype(F32)
    fx[0, 2:3, :] = tgt[...].astype(F32)
    line = {}
    for k in (1, 3, 2):
        r = 4 - k
        line[r] = remote(fx.at[0], fx.at[r], fs.at[r], fr.at[r], dev(dx=k))
        line[r].start()
        sent.append(line[r])

    def scale(r):
        if r:
            line[r].wait_recv()
        factor, at_target, target = (as_column(fx[r, i : i + 1, :]) for i in range(3))
        for half in (top, low):
            e = eb[r, half, :].astype(F32) if r else pb[0, half, :]
            g = jnp.where(lanes == target[half], at_target[half], e * factor[half])
            gall[r, half, :] = g.astype(BF16)

    pair, zd = {}, {}

    def send_pair(r, h):
        cols = pl.ds(h * 1024, 1024)
        d = remote(gt.at[r, :, oc, :, cols], rb.at[r, :, :, cols], ds_.at[r, h], dr.at[r, h], dev(core=oc))
        d.start()
        pair[r, h] = d
        sent.append(d)

    def block_product(h, *blocks):
        def step(n, carry):
            at = pl.ds(pl.multiple_of(n * 256, 256), 256)
            out = pl.ds(pl.multiple_of(n * 256 + h * 1024, 256), 256)
            lhs = jnp.concatenate([gall[r] for r in blocks], axis=0)
            res = jnp.dot(lhs, wt[h, :, at], preferred_element_type=F32)
            for i, r in enumerate(blocks):
                gt[r, :, :, :, out] = res[i * 256 : (i + 1) * 256].reshape(NZ, 2, 16, 256)
            return carry

        lax.fori_loop(0, 4, step, 0)
        for r in blocks:
            send_pair(r, h)

    def own_block(h):
        factor, at_target = (as_column(fx[0, i : i + 1, :]).reshape(NZ, 2, 16, 1) for i in range(2))
        for j in range(h * 4, h * 4 + 4):
            cols = slice(j * 256, j * 256 + 256)
            gt[0, :, :, :, cols] = gt[0, :, :, :, cols] * factor + vt[:, :, :, cols] * at_target
        send_pair(0, h)

    def slot(k, half):
        return 2 * k - 1 + half if k else 0

    def z_half(r, k, d, half):
        zz = (z + (4 - k if d == 0 else 4 + k)) % NZ
        cols = pl.ds(half * 1024, 1024)
        val = gt[r, zz, c, :, cols] + rb[r, zz, :, cols]
        if k > 1 or (k == 1 and half == d):
            zd[r, d, k - 1, half].wait_recv()
            val = val + unpack_flat(zr.at[r, d, slot(k - 1, half)], 16, 1024)
        if k == 4:
            return val
        at = slot(k, half)
        pack_flat(val, zs.at[r, d, at])
        cp = remote(
            zs.at[r, d, at], zr.at[r, d, at], zss.at[0], zrs.at[r, d, at], dev(dz=1 if d == 0 else -1)
        )
        cp.start()
        zd[r, d, k, half] = cp

    def z_step(r, k):
        if k < 4:
            for d in range(2):
                if k == 0:
                    pair[r, d].wait_recv()
                z_half(r, k, d, d)
        if k < 3:
            for d in range(2):
                z_half(r, k + 1, d, 1 - d)
        if k == 4:
            for half in (0, 1):
                other = zd[r, 1, 3, half]
                val = z_half(r, 4, 0, half)
                other.wait_recv()
                fin[r, :, half * 1024 : half * 1024 + 1024] = val + unpack_flat(zr.at[r, 1, slot(3, half)], 16, 1024)

    def weight_tile(f):
        h, at = f // 4, pl.ds((f % 4) * 256, 256)
        lhs = hbuf[h, :, :, at].reshape(1024, 256)
        rhs = gall[...].reshape(1024, 1024)
        out = lax.dot_general(lhs, rhs, (((0,), (0,)), ((), ())), preferred_element_type=F32)
        gw[f * 256 : (f + 1) * 256, :] = out.astype(BF16)

    a0.wait_recv()
    f0 = send_e(4, 3, 2, upper, RIGHT)
    b0.wait_recv()
    f1 = send_e(5, 1, 2, lower, LEFT)
    own_block(0)
    own_block(1)
    scale(0)
    z_step(0, 0)
    a1.wait_recv()
    scale(3)
    b1.wait_recv()
    scale(1)
    block_product(0, 3, 1)
    z_step(0, 1)
    block_product(1, 3, 1)
    f0.wait_recv()
    f1.wait_recv()
    scale(2)
    block_product(0, 2)
    z_step(3, 0)
    z_step(1, 0)
    block_product(1, 2)
    z_step(0, 2)
    z_step(2, 0)
    z_step(3, 1)
    z_step(1, 1)
    z_step(0, 3)
    z_step(2, 1)
    z_step(3, 2)
    weight_tile(0)
    z_step(1, 2)
    z_step(0, 4)
    z_step(2, 2)
    z_step(3, 3)
    weight_tile(1)
    z_step(1, 3)
    z_step(2, 3)
    weight_tile(2)
    z_step(3, 4)
    z_step(1, 4)
    z_step(2, 4)

    def held(k):
        return fin[(y + k - x + NX) % NX]

    home = []
    for k in (2, 1, 3):
        pack_flat(held(k), ys.at[k])
        d = remote(ys.at[k], yr.at[k], yss.at[k], yrs.at[k], dev(dy=k))
        d.start()
        sent.append(d)
        home.append((k, d))
    weight_tile(3)
    weight_tile(4)
    weight_tile(5)
    weight_tile(6)
    weight_tile(7)
    total = held(0)
    for k, d in home:
        d.wait_recv()
        total = total + unpack_flat(yr.at[k], 16, 2048)
    gh[...] = total.astype(BF16)

    def drain():
        for d in sent:
            d.wait_send()
        remote(zs, zr, zss.at[0], zrs.at[0, 0, 0], dev(dz=1)).wait_send()

    drain()


def finish(loss_in, gh_in, gw_in, loss, gh, gw, sem):
    pairs = ((gw_in, gw), (gh_in, gh), (loss_in, loss))
    copies = [pltpu.make_async_copy(a, b, sem.at[k]) for k, (a, b) in enumerate(pairs)]
    for d in copies:
        d.start()
    for d in copies:
        d.wait()


def shards(hidden, weight, targets, cotangent):
    args = (hidden, weight, targets.reshape(1, 256), cotangent.reshape(1, 256))
    vm, dma = pltpu.VMEM, pltpu.SemaphoreType.DMA
    space = pl.BlockSpec(memory_space=pltpu.VMEM)
    raw = pl.BlockSpec(memory_space=pl.ANY)
    loss, gh, gw = pl.pallas_call(
        kernel,
        out_shape=(
            jax.ShapeDtypeStruct((1, 256), F32),
            jax.ShapeDtypeStruct((16, 2048), BF16),
            jax.ShapeDtypeStruct((2048, 1024), BF16),
        ),
        in_specs=[pl.BlockSpec(memory_space=pltpu.HBM)] * 4,
        out_specs=(space, space, space),
        scratch_shapes=[
            vm((1, 256), jnp.int32),
            vm((1, 256), F32),
            vm((64, 1024), BF16),
            vm((2, 4, 256, 1024), BF16),
            vm((2, 1024, 1024), BF16),
            vm((2, 1024, 1024), BF16),
            vm((4, 256, 1024), F32),
            vm((6, 1040, 128), I16),
            vm((6, 1040, 128), I16),
            vm((4, 8, 8, 256), F32),
            vm((4, 256, 1024), BF16),
            vm((4, 8, 256), F32),
            vm((4, 256, 1024), BF16),
            vm((256, 1024), BF16),
            vm((NZ, 2, 16, 2048), F32),
            vm((4, NZ, 2, 16, 2048), F32),
            vm((4, NZ, 16, 2048), F32),
            vm((4, 2, 7, 144, 128), I16),
            vm((4, 2, 7, 144, 128), I16),
            vm((4, 16, 2048), F32),
            vm((4, 272, 128), I16),
            vm((4, 272, 128), I16),
            dma((7,)), dma((13,)), dma((13,)), dma((6,)), dma((6,)),
            dma((2, 8)), dma((2, 8)), dma((6,)), dma((6,)), dma((4,)), dma((4,)), dma((4, 2)), dma((4, 2)),
            dma((1,)), dma((4, 2, 7)), dma((4,)), dma((4,)),
        ],
        compiler_params=pltpu.CompilerParams(
            collective_id=0, has_side_effects=True, vmem_limit_bytes=49 * 1024 * 1024
        ),
    )(*(pltpu.with_memory_space_constraint(a, pltpu.HBM) for a in args))
    loss, gh, gw = pl.pallas_call(
        finish,
        out_shape=(
            jax.ShapeDtypeStruct((1, 256), F32),
            jax.ShapeDtypeStruct((16, 2048), BF16),
            jax.ShapeDtypeStruct((2048, 1024), BF16),
        ),
        in_specs=[space, space, space],
        out_specs=(raw, raw, raw),
        scratch_shapes=[dma((3,))],
        compiler_params=pltpu.CompilerParams(vmem_limit_bytes=8 * 1024 * 1024),
    )(loss, gh, gw)
    return loss.reshape(256), gh, gw


def solution(mesh):
    in_specs = (P("dp", None), P("dp", "vocab"), P("dp"), P("dp"))
    out_specs = (P("dp"), P("vocab", "dp"), P("dp", "vocab"))
    return jax.shard_map(shards, mesh=mesh, in_specs=in_specs, out_specs=out_specs, check_vma=False)
```

```python
import jax
import jax.numpy as jnp
from jax import lax
from jax.experimental import pallas as pl
from jax.experimental.pallas import tpu as pltpu
from jax.sharding import PartitionSpec as P

F32, BF16, I16 = jnp.float32, jnp.bfloat16, jnp.int16
NX, NY, NZ = 4, 4, 8
FINE = 64.0 / 0.6931471805599453
TOP = 32700.0


def row_code(x):
    top = jnp.max(jnp.abs(x), axis=1, keepdims=True)
    return jnp.ceil(jnp.log(jnp.maximum(top, 1e-30)) * FINE)


def pack_tall(x, dst):
    rows, cols = x.shape
    k = row_code(x)
    inv = jnp.exp(k * (-1.0 / FINE)) * TOP
    for j in range(cols // 128):
        dst[j * rows : (j + 1) * rows, :] = jnp.round(x[:, j * 128 : (j + 1) * 128] * inv).astype(I16)
    line = jnp.broadcast_to(k, (rows, 128)).T[0:1, :]
    dst[cols // 128 * rows : cols // 128 * rows + 16, :] = jnp.broadcast_to(line, (16, 128)).astype(I16)


def unpack_tall(src, rows, cols):
    at = cols // 128 * rows
    line = src[at : at + 16, :].astype(F32)[0:1, :]
    k = jnp.broadcast_to(line, (rows, rows)).T
    scale = jnp.exp(k * (1.0 / FINE)) * (1.0 / TOP)
    return jnp.concatenate(
        [src[j * rows : (j + 1) * rows, :].astype(F32) * scale for j in range(cols // 128)], axis=1
    )


def pack_flat(x, dst):
    rows, cols = x.shape
    k = row_code(x)
    inv = jnp.exp(k * (-1.0 / FINE)) * TOP
    for j in range(cols // 128):
        dst[j * rows : (j + 1) * rows, :] = jnp.round(x[:, j * 128 : (j + 1) * 128] * inv).astype(I16)
    dst[cols // 128 * rows : (cols // 128 + 1) * rows, :] = jnp.broadcast_to(k, (rows, 128)).astype(I16)


def unpack_flat(src, rows, cols):
    at = cols // 128 * rows
    scale = jnp.exp(src[at : at + rows, :].astype(F32) * (1.0 / FINE)) * (1.0 / TOP)
    return jnp.concatenate(
        [src[j * rows : (j + 1) * rows, :].astype(F32) * scale for j in range(cols // 128)], axis=1
    )


def pack_half(x, dst):
    k = row_code(x)
    inv = jnp.exp(k * (-1.0 / FINE)) * TOP
    for j in range(8):
        dst[j * 16 : (j + 1) * 16, :] = jnp.round(x[:, j * 128 : (j + 1) * 128] * inv).astype(I16)
    lower = lax.broadcasted_iota(jnp.int32, (8, 128), 1) < 64
    dst[128:136, :] = jnp.where(lower, k[:8], k[8:]).astype(I16)


def unpack_half(src):
    k = src[128:136, :].astype(F32)
    k = jnp.concatenate([k[:, 0:1], k[:, 64:65]], axis=0)
    scale = jnp.exp(k * (1.0 / FINE)) * (1.0 / TOP)
    return jnp.concatenate([src[j * 16 : (j + 1) * 16, :].astype(F32) * scale for j in range(8)], axis=1)


def as_column(line):
    n = line.shape[1]
    return jnp.broadcast_to(line, (128, n)).T[:, 0:1]


def as_line(column):
    n = column.shape[0]
    return jnp.broadcast_to(column, (n, 128)).T[0:1, :]


def kernel(
    hid, w, tgt_in, cot_in, loss, gh, gw,
    tgt, cot, xh,     hbuf, wbuf, wt, pb, sx, rx, st, eb, fx, gall, hot0, vt, gt, rb, zs, zr, fin, ys, yr,
    lsem, hs, hr, xs, xr, ss, sr, gs, gr, fs, fr, ds_, dr, zss, zrs, yss, yrs,
):
    x = lax.axis_index("dp")
    v = lax.axis_index("vocab")
    y, z, c = v // (2 * NZ), (v // 2) % NZ, v % 2
    oc = 1 - c

    def dev(dx=0, dy=0, dz=0, core=None):
        yy, zz = (y + dy) % NY, (z + dz) % NZ
        cc = c if core is None else core
        return {"dp": (x + dx) % NX, "vocab": (yy * NZ + zz) * 2 + cc}

    def remote(src, dst, send, recv, to):
        return pltpu.make_async_remote_copy(
            src_ref=src, dst_ref=dst, send_sem=send, recv_sem=recv,
            device_id=to, device_id_type=pl.DeviceIdType.MESH,
        )

    def columns_for(r):
        to = (4 - r) % 4
        return to, pl.ds(pl.multiple_of(((x + to) % NX) * 2048 + c * 1024, 1024), 1024)

    mine = pl.ds(pl.multiple_of(y * 64, 64), 64)
    far_to, far_cols = columns_for(2)
    ahead = pltpu.make_async_copy(hid.at[mine, far_cols], xh, lsem.at[6])
    ahead.start()

    local = [pltpu.make_async_copy(w.at[pl.ds(h * 1024, 1024), :], wbuf.at[h], lsem.at[h]) for h in range(2)]
    for h in range(2):
        cols = pl.multiple_of(x * 2048 + h * 1024, 1024)
        local.append(pltpu.make_async_copy(hid.at[:, pl.ds(cols, 1024)], hbuf.at[h, 0], lsem.at[2 + h]))
    local.append(pltpu.make_async_copy(tgt_in, tgt, lsem.at[4]))
    local.append(pltpu.make_async_copy(cot_in, cot, lsem.at[5]))
    for d in local:
        d.start()

    barrier = pltpu.get_barrier_semaphore()
    peers = [dev(dx=k) for k in (1, 2, 3)] + [dev(core=oc)]
    peers += [dev(dy=k, core=cc) for k in (1, 2, 3) for cc in (c, oc)] + [dev(dz=k) for k in range(1, NZ)]
    for p in peers:
        pl.semaphore_signal(barrier, inc=1, device_id=p, device_id_type=pl.DeviceIdType.MESH)
    pl.semaphore_wait(barrier, len(peers))

    sent = []
    take = {}
    ahead.wait()
    take[2] = remote(xh, hbuf.at[c, 2, mine, :], hs.at[0], hr.at[0], dev(dx=far_to))
    take[2].start()
    sent.append(take[2])

    def direct(r):
        to, cols = columns_for(r)
        take[r] = remote(hid.at[:, cols], hbuf.at[c, r], hs.at[r], hr.at[r], dev(dx=to))
        take[r].start()
        sent.append(take[r])

    around = {}

    def along_y(k, rows, dy):
        d = remote(hbuf.at[c, 2, rows, :], hbuf.at[c, 2, rows, :], hs.at[3 + k], hr.at[3 + k], dev(dy=dy))
        d.start()
        around[k] = d
        sent.append(d)

    def rows_of(dy, half):
        return pl.ds(pl.multiple_of(((y + dy) % NY) * 64 + half * 32, 32), 32)

    def spread():
        take[2].wait_recv()
        along_y(1, rows_of(0, 0), 1)
        along_y(2, rows_of(0, 1), -1)
        along_y(3, rows_of(0, 1), 1)
        along_y(4, rows_of(0, 0), -1)

    def forward():
        around[1].wait_recv()
        along_y(5, rows_of(-1, 0), 1)
        around[2].wait_recv()
        along_y(6, rows_of(1, 1), -1)

    across = {}

    def share(r):
        if r == 2:
            for k in (3, 4, 5, 6):
                around[k].wait_recv()
        else:
            take[r].wait_recv()
        d = remote(hbuf.at[c, r], hbuf.at[c, r], hs.at[9 + r], hr.at[9 + r], dev(core=oc))
        d.start()
        across[r] = d
        sent.append(d)

    def product(r, core, add):
        def step(n, carry):
            at = pl.ds(pl.multiple_of(n * 256, 256), 256)
            res = jnp.dot(hbuf[core, r], wbuf[core, :, at], preferred_element_type=F32)
            pb[r, :, at] = pb[r, :, at] + res if add else res
            return carry

        lax.fori_loop(0, 4, step, 0)

    def arrived(r):
        across[r].wait_recv()

    def turn(h):
        def step(n, carry):
            at = pl.ds(pl.multiple_of(n * 256, 256), 256)
            wt[h, :, at] = wbuf[h, at, :].T
            return carry

        lax.fori_loop(0, 4, step, 0)

    RIGHT, LEFT = 1, -1
    ring = {}

    def send_x(k, dx):
        d = remote(sx.at[k], rx.at[k], xs.at[k], xr.at[k], dev(dx=dx))
        d.start()
        ring[k] = d
        sent.append(d)

    top, low = slice(0, 128), slice(128, 256)
    spread()
    direct(1)
    direct(3)
    for d in local:
        d.wait()
    product(0, 0, False)
    forward()
    product(0, 1, True)
    share(2)
    product(2, c, False)
    arrived(2)
    product(2, oc, True)
    pack_tall(pb[2, top, :], sx.at[0])
    send_x(0, RIGHT)
    pack_tall(pb[2, low, :], sx.at[1])
    send_x(1, LEFT)
    share(1)
    share(3)
    product(1, c, False)
    arrived(1)
    product(1, oc, True)
    pack_tall(pb[1, low, :], sx.at[2])
    send_x(2, RIGHT)
    product(3, c, False)
    arrived(3)
    product(3, oc, True)
    pack_tall(pb[3, top, :], sx.at[3])
    send_x(3, LEFT)
    ring[0].wait_recv()
    pack_tall(pb[1, top, :] + unpack_tall(rx.at[0], 128, 1024), sx.at[4])
    send_x(4, RIGHT)
    ring[1].wait_recv()
    pack_tall(pb[3, low, :] + unpack_tall(rx.at[1], 128, 1024), sx.at[5])
    send_x(5, LEFT)
    turn(0)
    turn(1)
    ring[2].wait_recv()
    pb[0, low, :] += unpack_tall(rx.at[2], 128, 1024)
    ring[3].wait_recv()
    pb[0, top, :] += unpack_tall(rx.at[3], 128, 1024)
    ring[4].wait_recv()
    pb[0, top, :] += unpack_tall(rx.at[4], 128, 1024)
    ring[5].wait_recv()
    pb[0, low, :] += unpack_tall(rx.at[5], 128, 1024)

    target = as_column(tgt[...].astype(F32))
    first = (v * 1024).astype(F32)
    lanes = lax.broadcasted_iota(jnp.int32, (128, 1024), 1).astype(F32) + first

    def send_e(k, src, dst, half, dx):
        d = remote(eb.at[src, half, :], eb.at[dst, half, :], gs.at[k], gr.at[k], dev(dx=dx))
        d.start()
        sent.append(d)
        return d

    upper, lower = pl.ds(0, 128), pl.ds(128, 128)
    tops, sums, picks = [], [], []
    first_sends = []
    for half in (top, low):
        logit = pb[0, half, :]
        m = jnp.max(logit, axis=1, keepdims=True)
        hot = lanes == target[half]
        picks.append(jnp.sum(jnp.where(hot, logit, 0.0), axis=1, keepdims=True))
        e = jnp.exp(logit - m)
        eb[0, half, :] = e.astype(BF16)
        gall[0, half, :] = jnp.where(hot, 0.0, e).astype(BF16)
        hot0[half, :] = hot.astype(F32).astype(BF16)
        pb[0, half, :] = e
        tops.append(m)
        sums.append(jnp.sum(e, axis=1, keepdims=True))
        first_sends.append(send_e(0, 0, 3, upper, RIGHT) if half is top else send_e(1, 0, 1, lower, LEFT))
    a0, b0 = first_sends
    a1 = send_e(2, 0, 3, lower, RIGHT)
    b1 = send_e(3, 0, 1, upper, LEFT)
    st[0, 0, 0:1, :] = as_line(jnp.concatenate(tops, axis=0))
    st[0, 0, 1:2, :] = as_line(jnp.concatenate(sums, axis=0))
    st[0, 0, 2:3, :] = as_line(jnp.concatenate(picks, axis=0))

    def tell(level, places):
        out = []
        for k, p in enumerate(places, 1):
            d = remote(st.at[level, 0], st.at[level, k], ss.at[level, k], sr.at[level, k], p)
            d.start()
            sent.append(d)
            out.append(d)
        return out

    def join(level, told, out):
        for d in told:
            d.wait_recv()
        n = len(told) + 1
        m = st[level, 0, 0:1, :]
        for k in range(1, n):
            m = jnp.maximum(m, st[level, k, 0:1, :])
        s = jnp.zeros_like(m)
        q = jnp.zeros_like(m)
        for k in range(n):
            s = s + st[level, k, 1:2, :] * jnp.exp(st[level, k, 0:1, :] - m)
            q = q + st[level, k, 2:3, :]
        st[out, 0, 0:1, :] = m
        st[out, 0, 1:2, :] = s
        st[out, 0, 2:3, :] = q
        return m, s, q

    def row_product(lhs, out):
        def step(n, carry):
            at = pl.ds(pl.multiple_of((n % 4) * 256, 256), 256)
            to = pl.ds(pl.multiple_of(n * 256, 256), 256)
            res = jnp.dot(lhs[...], wt[n // 4, :, at], preferred_element_type=F32)
            out[:, :, :, to] = res.reshape(NZ, 2, 16, 256)
            return carry

        lax.fori_loop(0, 8, step, 0)

    told = tell(0, [dev(core=oc)] + [dev(dy=k, core=cc) for k in (1, 2, 3) for cc in (c, oc)])
    row_product(hot0, vt)
    join(0, told, 1)
    told = tell(1, [dev(dz=k) for k in range(1, NZ)])
    row_product(gall.at[0], gt.at[0])
    m, s, q = join(1, told, 2)
    loss[...] = m + jnp.log(s) - q
    weigh = cot[...]
    fx[0, 0:1, :] = weigh * (jnp.exp(st[0, 0, 0:1, :] - m) / s)
    fx[0, 1:2, :] = (weigh * (jnp.exp(q - m) / s - 1.0)).astype(BF16).astype(F32)
    fx[0, 2:3, :] = tgt[...].astype(F32)
    line = {}
    for k in (1, 3, 2):
        r = 4 - k
        line[r] = remote(fx.at[0], fx.at[r], fs.at[r], fr.at[r], dev(dx=k))
        line[r].start()
        sent.append(line[r])

    def scale(r):
        if r:
            line[r].wait_recv()
        factor, at_target, target = (as_column(fx[r, i : i + 1, :]) for i in range(3))
        for half in (top, low):
            e = eb[r, half, :].astype(F32) if r else pb[0, half, :]
            g = jnp.where(lanes == target[half], at_target[half], e * factor[half])
            gall[r, half, :] = g.astype(BF16)

    pair, zd = {}, {}

    def send_pair(r, h):
        cols = pl.ds(h * 1024, 1024)
        d = remote(gt.at[r, :, oc, :, cols], rb.at[r, :, :, cols], ds_.at[r, h], dr.at[r, h], dev(core=oc))
        d.start()
        pair[r, h] = d
        sent.append(d)

    def block_product(h, *blocks):
        def step(n, carry):
            at = pl.ds(pl.multiple_of(n * 256, 256), 256)
            out = pl.ds(pl.multiple_of(n * 256 + h * 1024, 256), 256)
            lhs = jnp.concatenate([gall[r] for r in blocks], axis=0)
            res = jnp.dot(lhs, wt[h, :, at], preferred_element_type=F32)
            for i, r in enumerate(blocks):
                gt[r, :, :, :, out] = res[i * 256 : (i + 1) * 256].reshape(NZ, 2, 16, 256)
            return carry

        lax.fori_loop(0, 4, step, 0)
        for r in blocks:
            send_pair(r, h)

    def own_block(h):
        factor, at_target = (as_column(fx[0, i : i + 1, :]).reshape(NZ, 2, 16, 1) for i in range(2))
        for j in range(h * 4, h * 4 + 4):
            cols = slice(j * 256, j * 256 + 256)
            gt[0, :, :, :, cols] = gt[0, :, :, :, cols] * factor + vt[:, :, :, cols] * at_target
        send_pair(0, h)

    def slot(k, half):
        return 2 * k - 1 + half if k else 0

    def z_half(r, k, d, half):
        zz = (z + (4 - k if d == 0 else 4 + k)) % NZ
        cols = pl.ds(half * 1024, 1024)
        val = gt[r, zz, c, :, cols] + rb[r, zz, :, cols]
        if k > 1 or (k == 1 and half == d):
            zd[r, d, k - 1, half].wait_recv()
            val = val + unpack_half(zr.at[r, d, slot(k - 1, half)])
        if k == 4:
            return val
        at = slot(k, half)
        pack_half(val, zs.at[r, d, at])
        cp = remote(
            zs.at[r, d, at], zr.at[r, d, at], zss.at[0], zrs.at[r, d, at], dev(dz=1 if d == 0 else -1)
        )
        cp.start()
        zd[r, d, k, half] = cp

    def z_step(r, k):
        if k < 4:
            for d in range(2):
                if k == 0:
                    pair[r, d].wait_recv()
                z_half(r, k, d, d)
        if k < 3:
            for d in range(2):
                z_half(r, k + 1, d, 1 - d)
        if k == 4:
            for half in (0, 1):
                other = zd[r, 1, 3, half]
                val = z_half(r, 4, 0, half)
                other.wait_recv()
                fin[r, :, half * 1024 : half * 1024 + 1024] = val + unpack_half(zr.at[r, 1, slot(3, half)])

    def weight_tile(f):
        h, at = f // 4, pl.ds((f % 4) * 256, 256)
        lhs = hbuf[h, :, :, at].reshape(1024, 256)
        rhs = gall[...].reshape(1024, 1024)
        out = lax.dot_general(lhs, rhs, (((0,), (0,)), ((), ())), preferred_element_type=F32)
        gw[f * 256 : (f + 1) * 256, :] = out.astype(BF16)

    a0.wait_recv()
    f0 = send_e(4, 3, 2, upper, RIGHT)
    b0.wait_recv()
    f1 = send_e(5, 1, 2, lower, LEFT)
    own_block(0)
    own_block(1)
    scale(0)
    z_step(0, 0)
    a1.wait_recv()
    scale(3)
    b1.wait_recv()
    scale(1)
    block_product(0, 3, 1)
    z_step(0, 1)
    block_product(1, 3, 1)
    f0.wait_recv()
    f1.wait_recv()
    scale(2)
    block_product(0, 2)
    z_step(3, 0)
    z_step(1, 0)
    block_product(1, 2)
    z_step(0, 2)
    z_step(2, 0)
    z_step(3, 1)
    z_step(1, 1)
    z_step(0, 3)
    z_step(2, 1)
    z_step(3, 2)
    weight_tile(0)
    z_step(1, 2)
    z_step(0, 4)
    z_step(2, 2)
    z_step(3, 3)
    weight_tile(1)
    z_step(1, 3)
    z_step(2, 3)
    weight_tile(2)
    z_step(3, 4)
    z_step(1, 4)
    z_step(2, 4)

    def held(k):
        return fin[(y + k - x + NX) % NX]

    home = []
    for k in (2, 1, 3):
        pack_flat(held(k), ys.at[k])
        d = remote(ys.at[k], yr.at[k], yss.at[k], yrs.at[k], dev(dy=k))
        d.start()
        sent.append(d)
        home.append((k, d))
    weight_tile(3)
    weight_tile(4)
    weight_tile(5)
    weight_tile(6)
    weight_tile(7)
    total = held(0)
    for k, d in home:
        d.wait_recv()
        total = total + unpack_flat(yr.at[k], 16, 2048)
    gh[...] = total.astype(BF16)

    def drain():
        for d in sent:
            d.wait_send()
        remote(zs, zr, zss.at[0], zrs.at[0, 0, 0], dev(dz=1)).wait_send()

    drain()


def finish(loss_in, gh_in, gw_in, loss, gh, gw, sem):
    pairs = ((gw_in, gw), (gh_in, gh), (loss_in, loss))
    copies = [pltpu.make_async_copy(a, b, sem.at[k]) for k, (a, b) in enumerate(pairs)]
    for d in copies:
        d.start()
    for d in copies:
        d.wait()


def shards(hidden, weight, targets, cotangent):
    args = (hidden, weight, targets.reshape(1, 256), cotangent.reshape(1, 256))
    vm, dma = pltpu.VMEM, pltpu.SemaphoreType.DMA
    space = pl.BlockSpec(memory_space=pltpu.VMEM)
    raw = pl.BlockSpec(memory_space=pl.ANY)
    loss, gh, gw = pl.pallas_call(
        kernel,
        out_shape=(
            jax.ShapeDtypeStruct((1, 256), F32),
            jax.ShapeDtypeStruct((16, 2048), BF16),
            jax.ShapeDtypeStruct((2048, 1024), BF16),
        ),
        in_specs=[pl.BlockSpec(memory_space=pltpu.HBM)] * 4,
        out_specs=(space, space, space),
        scratch_shapes=[
            vm((1, 256), jnp.int32),
            vm((1, 256), F32),
            vm((64, 1024), BF16),
            vm((2, 4, 256, 1024), BF16),
            vm((2, 1024, 1024), BF16),
            vm((2, 1024, 1024), BF16),
            vm((4, 256, 1024), F32),
            vm((6, 1040, 128), I16),
            vm((6, 1040, 128), I16),
            vm((4, 8, 8, 256), F32),
            vm((4, 256, 1024), BF16),
            vm((4, 8, 256), F32),
            vm((4, 256, 1024), BF16),
            vm((256, 1024), BF16),
            vm((NZ, 2, 16, 2048), F32),
            vm((4, NZ, 2, 16, 2048), F32),
            vm((4, NZ, 16, 2048), F32),
            vm((4, 2, 7, 136, 128), I16),
            vm((4, 2, 7, 136, 128), I16),
            vm((4, 16, 2048), F32),
            vm((4, 272, 128), I16),
            vm((4, 272, 128), I16),
            dma((7,)), dma((13,)), dma((13,)), dma((6,)), dma((6,)),
            dma((2, 8)), dma((2, 8)), dma((6,)), dma((6,)), dma((4,)), dma((4,)), dma((4, 2)), dma((4, 2)),
            dma((1,)), dma((4, 2, 7)), dma((4,)), dma((4,)),
        ],
        compiler_params=pltpu.CompilerParams(
            collective_id=0, has_side_effects=True, vmem_limit_bytes=49 * 1024 * 1024
        ),
    )(*(pltpu.with_memory_space_constraint(a, pltpu.HBM) for a in args))
    loss, gh, gw = pl.pallas_call(
        finish,
        out_shape=(
            jax.ShapeDtypeStruct((1, 256), F32),
            jax.ShapeDtypeStruct((16, 2048), BF16),
            jax.ShapeDtypeStruct((2048, 1024), BF16),
        ),
        in_specs=[space, space, space],
        out_specs=(raw, raw, raw),
        scratch_shapes=[dma((3,))],
        compiler_params=pltpu.CompilerParams(vmem_limit_bytes=8 * 1024 * 1024),
    )(loss, gh, gw)
    return loss.reshape(256), gh, gw


def solution(mesh):
    in_specs = (P("dp", None), P("dp", "vocab"), P("dp"), P("dp"))
    out_specs = (P("dp"), P("vocab", "dp"), P("dp", "vocab"))
    return jax.shard_map(shards, mesh=mesh, in_specs=in_specs, out_specs=out_specs, check_vma=False)
```

```python
import jax
import jax.numpy as jnp
from jax import lax
from jax.experimental import pallas as pl
from jax.experimental.pallas import tpu as pltpu
from jax.sharding import PartitionSpec as P

F32, BF16, I16 = jnp.float32, jnp.bfloat16, jnp.int16
NX, NY, NZ = 4, 4, 8
FINE = 64.0 / 0.6931471805599453
TOP = 32700.0


def row_code(x):
    top = jnp.max(jnp.abs(x), axis=1, keepdims=True)
    return jnp.ceil(jnp.log(jnp.maximum(top, 1e-30)) * FINE)


def pack_tall(x, dst):
    rows, cols = x.shape
    k = row_code(x)
    inv = jnp.exp(k * (-1.0 / FINE)) * TOP
    for j in range(cols // 128):
        dst[j * rows : (j + 1) * rows, :] = jnp.round(x[:, j * 128 : (j + 1) * 128] * inv).astype(I16)
    line = jnp.broadcast_to(k, (rows, 128)).T[0:1, :]
    dst[cols // 128 * rows : cols // 128 * rows + 16, :] = jnp.broadcast_to(line, (16, 128)).astype(I16)


def unpack_tall(src, rows, cols):
    at = cols // 128 * rows
    line = src[at : at + 16, :].astype(F32)[0:1, :]
    k = jnp.broadcast_to(line, (rows, rows)).T
    scale = jnp.exp(k * (1.0 / FINE)) * (1.0 / TOP)
    return jnp.concatenate(
        [src[j * rows : (j + 1) * rows, :].astype(F32) * scale for j in range(cols // 128)], axis=1
    )


def pack_flat(x, dst):
    rows, cols = x.shape
    k = row_code(x)
    inv = jnp.exp(k * (-1.0 / FINE)) * TOP
    for j in range(cols // 128):
        dst[j * rows : (j + 1) * rows, :] = jnp.round(x[:, j * 128 : (j + 1) * 128] * inv).astype(I16)
    dst[cols // 128 * rows : (cols // 128 + 1) * rows, :] = jnp.broadcast_to(k, (rows, 128)).astype(I16)


def unpack_flat(src, rows, cols):
    at = cols // 128 * rows
    scale = jnp.exp(src[at : at + rows, :].astype(F32) * (1.0 / FINE)) * (1.0 / TOP)
    return jnp.concatenate(
        [src[j * rows : (j + 1) * rows, :].astype(F32) * scale for j in range(cols // 128)], axis=1
    )


def pack_half(x, dst):
    k = row_code(x)
    inv = jnp.exp(k * (-1.0 / FINE)) * TOP
    for j in range(8):
        dst[j * 16 : (j + 1) * 16, :] = jnp.round(x[:, j * 128 : (j + 1) * 128] * inv).astype(I16)
    lower = lax.broadcasted_iota(jnp.int32, (8, 128), 1) < 64
    dst[128:136, :] = jnp.where(lower, k[:8], k[8:]).astype(I16)


def unpack_half(src):
    k = src[128:136, :].astype(F32)
    k = jnp.concatenate([k[:, 0:1], k[:, 64:65]], axis=0)
    scale = jnp.exp(k * (1.0 / FINE)) * (1.0 / TOP)
    return jnp.concatenate([src[j * 16 : (j + 1) * 16, :].astype(F32) * scale for j in range(8)], axis=1)


def as_column(line):
    n = line.shape[1]
    return jnp.broadcast_to(line, (128, n)).T[:, 0:1]


def as_line(column):
    n = column.shape[0]
    return jnp.broadcast_to(column, (n, 128)).T[0:1, :]


def kernel(
    hid, w, tgt_in, cot_in, loss, gh, gw,
    tgt, cot, xh,     hbuf, wbuf, wt, pb, sx, rx, st, eb, fx, gall, hot0, vt, gt, rb, zs, zr, fin, ys, yr,
    lsem, hs, hr, xs, xr, ss, sr, gs, gr, fs, fr, ds_, dr, zss, zrs, yss, yrs,
):
    x = lax.axis_index("dp")
    v = lax.axis_index("vocab")
    y, z, c = v // (2 * NZ), (v // 2) % NZ, v % 2
    oc = 1 - c

    def dev(dx=0, dy=0, dz=0, core=None):
        yy, zz = (y + dy) % NY, (z + dz) % NZ
        cc = c if core is None else core
        return {"dp": (x + dx) % NX, "vocab": (yy * NZ + zz) * 2 + cc}

    def remote(src, dst, send, recv, to):
        return pltpu.make_async_remote_copy(
            src_ref=src, dst_ref=dst, send_sem=send, recv_sem=recv,
            device_id=to, device_id_type=pl.DeviceIdType.MESH,
        )

    def columns_for(r):
        to = (4 - r) % 4
        return to, pl.ds(pl.multiple_of(((x + to) % NX) * 2048 + c * 1024, 1024), 1024)

    mine = pl.ds(pl.multiple_of(y * 64, 64), 64)
    far_to, far_cols = columns_for(2)
    ahead = pltpu.make_async_copy(hid.at[mine, far_cols], xh, lsem.at[6])
    ahead.start()

    local = [pltpu.make_async_copy(w.at[pl.ds(h * 1024, 1024), :], wbuf.at[h], lsem.at[h]) for h in range(2)]
    for h in range(2):
        cols = pl.multiple_of(x * 2048 + h * 1024, 1024)
        local.append(pltpu.make_async_copy(hid.at[:, pl.ds(cols, 1024)], hbuf.at[h, 0], lsem.at[2 + h]))
    local.append(pltpu.make_async_copy(tgt_in, tgt, lsem.at[4]))
    local.append(pltpu.make_async_copy(cot_in, cot, lsem.at[5]))
    for d in local:
        d.start()

    barrier = pltpu.get_barrier_semaphore()
    peers = [dev(dx=k) for k in (1, 2, 3)] + [dev(core=oc)]
    peers += [dev(dy=k, core=cc) for k in (1, 2, 3) for cc in (c, oc)] + [dev(dz=k) for k in range(1, NZ)]
    for p in peers:
        pl.semaphore_signal(barrier, inc=1, device_id=p, device_id_type=pl.DeviceIdType.MESH)
    pl.semaphore_wait(barrier, len(peers))

    sent = []
    take = {}
    ahead.wait()
    take[2] = remote(xh, hbuf.at[c, 2, mine, :], hs.at[0], hr.at[0], dev(dx=far_to))
    take[2].start()
    sent.append(take[2])

    def direct(r):
        to, cols = columns_for(r)
        take[r] = remote(hid.at[:, cols], hbuf.at[c, r], hs.at[r], hr.at[r], dev(dx=to))
        take[r].start()
        sent.append(take[r])

    around = {}

    def along_y(k, rows, dy):
        d = remote(hbuf.at[c, 2, rows, :], hbuf.at[c, 2, rows, :], hs.at[3 + k], hr.at[3 + k], dev(dy=dy))
        d.start()
        around[k] = d
        sent.append(d)

    def rows_of(dy, half):
        return pl.ds(pl.multiple_of(((y + dy) % NY) * 64 + half * 32, 32), 32)

    def spread():
        take[2].wait_recv()
        along_y(1, rows_of(0, 0), 1)
        along_y(2, rows_of(0, 1), -1)
        along_y(3, rows_of(0, 1), 1)
        along_y(4, rows_of(0, 0), -1)

    def forward():
        around[1].wait_recv()
        along_y(5, rows_of(-1, 0), 1)
        around[2].wait_recv()
        along_y(6, rows_of(1, 1), -1)

    across = {}

    def share(r):
        if r == 2:
            for k in (3, 4, 5, 6):
                around[k].wait_recv()
        else:
            take[r].wait_recv()
        d = remote(hbuf.at[c, r], hbuf.at[c, r], hs.at[9 + r], hr.at[9 + r], dev(core=oc))
        d.start()
        across[r] = d
        sent.append(d)

    def product(r, core, add):
        def step(n, carry):
            at = pl.ds(pl.multiple_of(n * 256, 256), 256)
            res = jnp.dot(hbuf[core, r], wbuf[core, :, at], preferred_element_type=F32)
            pb[r, :, at] = pb[r, :, at] + res if add else res
            return carry

        lax.fori_loop(0, 4, step, 0)

    def arrived(r):
        across[r].wait_recv()

    def turn(h):
        def step(n, carry):
            at = pl.ds(pl.multiple_of(n * 256, 256), 256)
            wt[h, :, at] = wbuf[h, at, :].T
            return carry

        lax.fori_loop(0, 4, step, 0)

    RIGHT, LEFT = 1, -1
    ring = {}

    def send_x(k, dx):
        d = remote(sx.at[k], rx.at[k], xs.at[0], xr.at[k], dev(dx=dx))
        d.start()
        ring[k] = d

    top, low = slice(0, 128), slice(128, 256)
    spread()
    direct(1)
    direct(3)
    for d in local:
        d.wait()
    product(0, 0, False)
    forward()
    product(0, 1, True)
    share(2)
    product(2, c, False)
    arrived(2)
    product(2, oc, True)
    pack_tall(pb[2, top, :], sx.at[0])
    send_x(0, RIGHT)
    pack_tall(pb[2, low, :], sx.at[1])
    send_x(1, LEFT)
    share(1)
    share(3)
    product(1, c, False)
    arrived(1)
    product(1, oc, True)
    pack_tall(pb[1, low, :], sx.at[2])
    send_x(2, RIGHT)
    product(3, c, False)
    arrived(3)
    product(3, oc, True)
    pack_tall(pb[3, top, :], sx.at[3])
    send_x(3, LEFT)
    ring[0].wait_recv()
    pack_tall(pb[1, top, :] + unpack_tall(rx.at[0], 128, 1024), sx.at[4])
    send_x(4, RIGHT)
    ring[1].wait_recv()
    pack_tall(pb[3, low, :] + unpack_tall(rx.at[1], 128, 1024), sx.at[5])
    send_x(5, LEFT)
    turn(0)
    turn(1)
    ring[2].wait_recv()
    pb[0, low, :] += unpack_tall(rx.at[2], 128, 1024)
    ring[3].wait_recv()
    pb[0, top, :] += unpack_tall(rx.at[3], 128, 1024)
    ring[4].wait_recv()
    pb[0, top, :] += unpack_tall(rx.at[4], 128, 1024)
    ring[5].wait_recv()
    pb[0, low, :] += unpack_tall(rx.at[5], 128, 1024)

    target = as_column(tgt[...].astype(F32))
    first = (v * 1024).astype(F32)
    lanes = lax.broadcasted_iota(jnp.int32, (128, 1024), 1).astype(F32) + first

    def send_e(k, src, dst, half, dx):
        d = remote(eb.at[src, half, :], eb.at[dst, half, :], gs.at[0], gr.at[k], dev(dx=dx))
        d.start()
        return d

    upper, lower = pl.ds(0, 128), pl.ds(128, 128)
    tops, sums, picks = [], [], []
    first_sends = []
    for half in (top, low):
        logit = pb[0, half, :]
        m = jnp.max(logit, axis=1, keepdims=True)
        hot = lanes == target[half]
        picks.append(jnp.sum(jnp.where(hot, logit, 0.0), axis=1, keepdims=True))
        e = jnp.exp(logit - m)
        eb[0, half, :] = e.astype(BF16)
        gall[0, half, :] = jnp.where(hot, 0.0, e).astype(BF16)
        hot0[half, :] = hot.astype(F32).astype(BF16)
        pb[0, half, :] = e
        tops.append(m)
        sums.append(jnp.sum(e, axis=1, keepdims=True))
        first_sends.append(send_e(0, 0, 3, upper, RIGHT) if half is top else send_e(1, 0, 1, lower, LEFT))
    a0, b0 = first_sends
    a1 = send_e(2, 0, 3, lower, RIGHT)
    b1 = send_e(3, 0, 1, upper, LEFT)
    st[0, 0, 0:1, :] = as_line(jnp.concatenate(tops, axis=0))
    st[0, 0, 1:2, :] = as_line(jnp.concatenate(sums, axis=0))
    st[0, 0, 2:3, :] = as_line(jnp.concatenate(picks, axis=0))

    def tell(level, places):
        out = []
        for k, p in enumerate(places, 1):
            d = remote(st.at[level, 0], st.at[level, k], ss.at[0], sr.at[level, k], p)
            d.start()
            out.append(d)
        return out

    def join(level, told, out):
        for d in told:
            d.wait_recv()
        n = len(told) + 1
        m = st[level, 0, 0:1, :]
        for k in range(1, n):
            m = jnp.maximum(m, st[level, k, 0:1, :])
        s = jnp.zeros_like(m)
        q = jnp.zeros_like(m)
        for k in range(n):
            s = s + st[level, k, 1:2, :] * jnp.exp(st[level, k, 0:1, :] - m)
            q = q + st[level, k, 2:3, :]
        st[out, 0, 0:1, :] = m
        st[out, 0, 1:2, :] = s
        st[out, 0, 2:3, :] = q
        return m, s, q

    def row_product(lhs, out):
        def step(n, carry):
            at = pl.ds(pl.multiple_of((n % 4) * 256, 256), 256)
            to = pl.ds(pl.multiple_of(n * 256, 256), 256)
            res = jnp.dot(lhs[...], wt[n // 4, :, at], preferred_element_type=F32)
            out[:, :, :, to] = res.reshape(NZ, 2, 16, 256)
            return carry

        lax.fori_loop(0, 8, step, 0)

    told = tell(0, [dev(core=oc)] + [dev(dy=k, core=cc) for k in (1, 2, 3) for cc in (c, oc)])
    row_product(hot0, vt)
    join(0, told, 1)
    told = tell(1, [dev(dz=k) for k in range(1, NZ)])
    row_product(gall.at[0], gt.at[0])
    m, s, q = join(1, told, 2)
    loss[...] = m + jnp.log(s) - q
    weigh = cot[...]
    fx[0, 0:1, :] = weigh * (jnp.exp(st[0, 0, 0:1, :] - m) / s)
    fx[0, 1:2, :] = (weigh * (jnp.exp(q - m) / s - 1.0)).astype(BF16).astype(F32)
    fx[0, 2:3, :] = tgt[...].astype(F32)
    line = {}
    for k in (1, 3, 2):
        r = 4 - k
        line[r] = remote(fx.at[0], fx.at[r], fs.at[r], fr.at[r], dev(dx=k))
        line[r].start()
        sent.append(line[r])

    def scale(r):
        if r:
            line[r].wait_recv()
        factor, at_target, target = (as_column(fx[r, i : i + 1, :]) for i in range(3))
        for half in (top, low):
            e = eb[r, half, :].astype(F32) if r else pb[0, half, :]
            g = jnp.where(lanes == target[half], at_target[half], e * factor[half])
            gall[r, half, :] = g.astype(BF16)

    pair, zd = {}, {}

    def send_pair(r, h):
        cols = pl.ds(h * 1024, 1024)
        d = remote(gt.at[r, :, oc, :, cols], rb.at[r, :, :, cols], ds_.at[0], dr.at[r, h], dev(core=oc))
        d.start()
        pair[r, h] = d

    def block_product(h, *blocks):
        def step(n, carry):
            at = pl.ds(pl.multiple_of(n * 256, 256), 256)
            out = pl.ds(pl.multiple_of(n * 256 + h * 1024, 256), 256)
            lhs = jnp.concatenate([gall[r] for r in blocks], axis=0)
            res = jnp.dot(lhs, wt[h, :, at], preferred_element_type=F32)
            for i, r in enumerate(blocks):
                gt[r, :, :, :, out] = res[i * 256 : (i + 1) * 256].reshape(NZ, 2, 16, 256)
            return carry

        lax.fori_loop(0, 4, step, 0)
        for r in blocks:
            send_pair(r, h)

    def own_block(h):
        factor, at_target = (as_column(fx[0, i : i + 1, :]).reshape(NZ, 2, 16, 1) for i in range(2))
        for j in range(h * 4, h * 4 + 4):
            cols = slice(j * 256, j * 256 + 256)
            gt[0, :, :, :, cols] = gt[0, :, :, :, cols] * factor + vt[:, :, :, cols] * at_target
        send_pair(0, h)

    def slot(k, half):
        return 2 * k - 1 + half if k else 0

    def z_half(r, k, d, half):
        zz = (z + (4 - k if d == 0 else 4 + k)) % NZ
        cols = pl.ds(half * 1024, 1024)
        val = gt[r, zz, c, :, cols] + rb[r, zz, :, cols]
        if k > 1 or (k == 1 and half == d):
            zd[r, d, k - 1, half].wait_recv()
            val = val + unpack_half(zr.at[r, d, slot(k - 1, half)])
        if k == 4:
            return val
        at = slot(k, half)
        pack_half(val, zs.at[r, d, at])
        cp = remote(
            zs.at[r, d, at], zr.at[r, d, at], zss.at[0], zrs.at[r, d, at], dev(dz=1 if d == 0 else -1)
        )
        cp.start()
        zd[r, d, k, half] = cp

    def z_step(r, k):
        if k < 4:
            for d in range(2):
                if k == 0:
                    pair[r, d].wait_recv()
                z_half(r, k, d, d)
        if k < 3:
            for d in range(2):
                z_half(r, k + 1, d, 1 - d)
        if k == 4:
            for half in (0, 1):
                other = zd[r, 1, 3, half]
                val = z_half(r, 4, 0, half)
                other.wait_recv()
                fin[r, :, half * 1024 : half * 1024 + 1024] = val + unpack_half(zr.at[r, 1, slot(3, half)])

    def weight_tile(f):
        h, at = f // 4, pl.ds((f % 4) * 256, 256)
        lhs = hbuf[h, :, :, at].reshape(1024, 256)
        rhs = gall[...].reshape(1024, 1024)
        out = lax.dot_general(lhs, rhs, (((0,), (0,)), ((), ())), preferred_element_type=F32)
        gw[f * 256 : (f + 1) * 256, :] = out.astype(BF16)

    a0.wait_recv()
    f0 = send_e(4, 3, 2, upper, RIGHT)
    b0.wait_recv()
    f1 = send_e(5, 1, 2, lower, LEFT)
    own_block(0)
    own_block(1)
    scale(0)
    z_step(0, 0)
    a1.wait_recv()
    scale(3)
    b1.wait_recv()
    scale(1)
    block_product(0, 3, 1)
    z_step(0, 1)
    block_product(1, 3, 1)
    f0.wait_recv()
    f1.wait_recv()
    scale(2)
    block_product(0, 2)
    z_step(3, 0)
    z_step(1, 0)
    block_product(1, 2)
    z_step(0, 2)
    z_step(2, 0)
    z_step(3, 1)
    z_step(1, 1)
    z_step(0, 3)
    z_step(2, 1)
    z_step(3, 2)
    weight_tile(0)
    z_step(1, 2)
    z_step(0, 4)
    z_step(2, 2)
    z_step(3, 3)
    weight_tile(1)
    z_step(1, 3)
    z_step(2, 3)
    weight_tile(2)
    z_step(3, 4)
    z_step(1, 4)
    z_step(2, 4)

    def held(k):
        return fin[(y + k - x + NX) % NX]

    home = []
    for k in (2, 1, 3):
        pack_flat(held(k), ys.at[k])
        d = remote(ys.at[k], yr.at[k], yss.at[k], yrs.at[k], dev(dy=k))
        d.start()
        sent.append(d)
        home.append((k, d))
    weight_tile(3)
    weight_tile(4)
    weight_tile(5)
    weight_tile(6)
    weight_tile(7)
    total = held(0)
    for k, d in home:
        d.wait_recv()
        total = total + unpack_flat(yr.at[k], 16, 2048)
    gh[...] = total.astype(BF16)

    def drain():
        for d in sent:
            d.wait_send()
        remote(zs, zr, zss.at[0], zrs.at[0, 0, 0], dev(dz=1)).wait_send()
        remote(rb, rb, ds_.at[0], dr.at[0, 0], dev(core=oc)).wait_send()
        remote(sx, rx, xs.at[0], xr.at[0], dev(dx=1)).wait_send()
        stats = st.at[pl.ds(0, 2), pl.ds(0, 7)]
        remote(stats, stats, ss.at[0], sr.at[0, 0], dev(dz=1)).wait_send()
        three = eb.at[pl.ds(0, 3)]
        remote(three, three, gs.at[0], gr.at[0], dev(dx=1)).wait_send()

    drain()


def finish(loss_in, gh_in, gw_in, loss, gh, gw, sem):
    pairs = ((gw_in, gw), (gh_in, gh), (loss_in, loss))
    copies = [pltpu.make_async_copy(a, b, sem.at[k]) for k, (a, b) in enumerate(pairs)]
    for d in copies:
        d.start()
    for d in copies:
        d.wait()


def shards(hidden, weight, targets, cotangent):
    args = (hidden, weight, targets.reshape(1, 256), cotangent.reshape(1, 256))
    vm, dma = pltpu.VMEM, pltpu.SemaphoreType.DMA
    space = pl.BlockSpec(memory_space=pltpu.VMEM)
    raw = pl.BlockSpec(memory_space=pl.ANY)
    loss, gh, gw = pl.pallas_call(
        kernel,
        out_shape=(
            jax.ShapeDtypeStruct((1, 256), F32),
            jax.ShapeDtypeStruct((16, 2048), BF16),
            jax.ShapeDtypeStruct((2048, 1024), BF16),
        ),
        in_specs=[pl.BlockSpec(memory_space=pltpu.HBM)] * 4,
        out_specs=(space, space, space),
        scratch_shapes=[
            vm((1, 256), jnp.int32),
            vm((1, 256), F32),
            vm((64, 1024), BF16),
            vm((2, 4, 256, 1024), BF16),
            vm((2, 1024, 1024), BF16),
            vm((2, 1024, 1024), BF16),
            vm((4, 256, 1024), F32),
            vm((6, 1040, 128), I16),
            vm((6, 1040, 128), I16),
            vm((4, 8, 8, 256), F32),
            vm((4, 256, 1024), BF16),
            vm((4, 8, 256), F32),
            vm((4, 256, 1024), BF16),
            vm((256, 1024), BF16),
            vm((NZ, 2, 16, 2048), F32),
            vm((4, NZ, 2, 16, 2048), F32),
            vm((4, NZ, 16, 2048), F32),
            vm((4, 2, 7, 136, 128), I16),
            vm((4, 2, 7, 136, 128), I16),
            vm((4, 16, 2048), F32),
            vm((4, 272, 128), I16),
            vm((4, 272, 128), I16),
            dma((7,)), dma((13,)), dma((13,)), dma((1,)), dma((6,)),
            dma((1,)), dma((2, 8)), dma((1,)), dma((6,)), dma((4,)), dma((4,)), dma((1,)), dma((4, 2)),
            dma((1,)), dma((4, 2, 7)), dma((4,)), dma((4,)),
        ],
        compiler_params=pltpu.CompilerParams(
            collective_id=0, has_side_effects=True, vmem_limit_bytes=49 * 1024 * 1024
        ),
    )(*(pltpu.with_memory_space_constraint(a, pltpu.HBM) for a in args))
    loss, gh, gw = pl.pallas_call(
        finish,
        out_shape=(
            jax.ShapeDtypeStruct((1, 256), F32),
            jax.ShapeDtypeStruct((16, 2048), BF16),
            jax.ShapeDtypeStruct((2048, 1024), BF16),
        ),
        in_specs=[space, space, space],
        out_specs=(raw, raw, raw),
        scratch_shapes=[dma((3,))],
        compiler_params=pltpu.CompilerParams(vmem_limit_bytes=8 * 1024 * 1024),
    )(loss, gh, gw)
    return loss.reshape(256), gh, gw


def solution(mesh):
    in_specs = (P("dp", None), P("dp", "vocab"), P("dp"), P("dp"))
    out_specs = (P("dp"), P("vocab", "dp"), P("dp", "vocab"))
    return jax.shard_map(shards, mesh=mesh, in_specs=in_specs, out_specs=out_specs, check_vma=False)
```
